32 devices in a mesh: band: 8 (over z, x), slab: 4 (over y, core).
Axes of the slice: x: 2, y: 2, z: 4, core: 2. Of those that a mesh axis runs over, the one named last changes fastest.
Arguments:
- orbitals: float32 [512, 64, 512], P('band', 'slab'), may hold values from -6 to 6
- potential: float32 [64, 512], P('slab'), may hold values from 0 to 1
- projectors: float32 [4, 2048, 128], replicated, may hold values from -0.125 to 0.125
- atom_kind: int32 [32], P('slab'), may hold values from 0 to 3
- atom_plane: int32 [32], P('slab'), may hold values from 0 to 60, as said below
- atom_coef: float32 [32, 128], P('slab'), may hold values from 0.2 to 1
- filter_cut: float32 [1], replicated, may hold values from 0.5 to 2
- filter_top: float32 [1], replicated, may hold values from 9 to 14
Outputs:
- new_orbitals: float32 [512, 32768], P(None, ('slab', 'band'))
The draws below stay inside these ranges and needn't reach their ends.
Inputs may be any that keep to these rules, and one draw needn't show every extreme that they name: `atom_plane`: block i's 4 planes lie inside the slab of planes (i // 8) * 16 to (i // 8 + 1) * 16 - 1; blocks may share planes.
All inputs are finite; a program needn't handle non-finite values.
Results may differ from the reference program's by a relative error of at most 0.0003.
Values sent between devices are 32-bit elements; how exact they have to be, the bound alone decides.
A program may use at most 128 MiB of HBM per device.

```python
import math
import jax
import jax.numpy as jnp
from jax import lax

NB = 512
FUNCS = 128
CX = 16
GY = 16
GZ = 32
BP = 4
KINDS = 4
ATOM_SLAB = 8
ORDER = 6
GX = 64
NPTS = 32768
ATOMS = 32
BPTS = 2048


def draw_atom_plane(key, part):
    atom_ids = jnp.arange(ATOMS).astype(jnp.int32)
    slab_ids = atom_ids // ATOM_SLAB
    offsets = jax.random.randint(key, (ATOMS,), 0, CX - BP + 1).astype(jnp.int32)
    return (slab_ids * CX + offsets).astype(jnp.int32)


def set_ends(array, key, least, largest):
    longest = array.shape.index(max(array.shape))
    spots = []
    for shift in (0, 1):
        where = [jax.random.randint(jax.random.fold_in(key, axis), (), 0, length) for axis, length in enumerate(array.shape)]
        where[longest] = (where[longest] + shift) % array.shape[longest]
        spots.append(tuple(where))
    return array.at[spots[0]].set(least).at[spots[1]].set(largest)


def block_levels(stream_key, extent, split, least, high):
    loudness, own = 1.0, jax.random.fold_in(stream_key, 6)
    for dim, parts in split:
        steps = jnp.exp(jax.random.uniform(jax.random.fold_in(own, dim), (parts,), jnp.float32, least / len(split), high / len(split)))
        loudness = loudness * jnp.repeat(steps, extent[dim] // parts).reshape([-1 if axis == dim else 1 for axis in range(len(extent))])
    return loudness


def bell_draw(key, shape, deviation, limit, pieces=(), held_as=jnp.bfloat16):
    entries = deviation * jax.random.normal(key, shape, jnp.float32)
    if pieces:
        entries = entries * block_levels(key, shape, pieces, -0.22, 0.18)
    return jnp.clip(entries, -limit, limit).astype(held_as)


def setup_inputs(seed: int = 0) -> dict:
    splits = jax.random.split(jax.random.key(seed), 9)
    return {
        "orbitals": bell_draw(splits[0], (NB, GX, GY * GZ), 1.0, 6.0, ((0, 8), (1, 4)), jnp.float32),
        "potential": jnp.clip(1.0 * jax.random.uniform(splits[1], (GX, GY * GZ), jnp.float32) ** block_levels(splits[1], (GX, GY * GZ), ((0, 4),), -0.2, 0.2), 0.0, 1.0),
        "projectors": bell_draw(splits[2], (KINDS, BPTS, FUNCS), BPTS ** -0.5, 0.125, (), jnp.float32),
        "atom_kind": set_ends(jax.random.randint(splits[3], (ATOMS,), 0, KINDS), jax.random.fold_in(splits[3], 1), 0, KINDS - 1).astype(jnp.int32),
        "atom_plane": draw_atom_plane(jax.random.fold_in(splits[8], 71), 0),
        "atom_coef": jnp.clip(jnp.exp(math.log(1.0) - 1.609438 * jax.random.uniform(splits[5], (ATOMS, FUNCS), jnp.float32) ** block_levels(splits[5], (ATOMS, FUNCS), ((0, 4),), -0.2, 0.2)), 0.2, 1.0),
        "filter_cut": jnp.clip(jax.random.uniform(splits[6], (1,), jnp.float32, 0.5, 2.0), 0.5, 2.0),
        "filter_top": jnp.clip(jax.random.uniform(splits[7], (1,), jnp.float32, 9.0, 14.0), 9.0, 14.0),
    }


low_edge = -1.0
near_coef = 4.0 / 3.0
far_coef = -1.0 / 12.0
self_coef = -2.5
highest = lax.Precision.HIGHEST

def shifted(source, offset):
    if offset > 0:
        zeros_part = jnp.zeros(source.shape[:-1] + (offset,), source.dtype)
        return jnp.concatenate([zeros_part, source[..., :-offset]], axis=-1)
    zeros_part = jnp.zeros(source.shape[:-1] + (-offset,), source.dtype)
    return jnp.concatenate([source[..., -offset:], zeros_part], axis=-1)

def transverse(source, width_z):
    length_last = source.shape[-1]
    z_position = jnp.arange(length_last) % width_z
    result_sum = 2.0 * self_coef * source
    for offset, weight_coef in ((1, near_coef), (-1, near_coef), (2, far_coef), (-2, far_coef)):
        result_sum = result_sum + weight_coef * shifted(source, offset * width_z)
        inside = (z_position - offset >= 0) & (z_position - offset < width_z)
        result_sum = result_sum + weight_coef * jnp.where(inside, shifted(source, offset), 0.0)
    return result_sum

def hamiltonian(source, potential, selector, atom_tables, atom_coef):
    along_x = self_coef * source
    along_x = along_x + near_coef * (jnp.roll(source, 1, axis=1) + jnp.roll(source, -1, axis=1))
    along_x = along_x + far_coef * (jnp.roll(source, 2, axis=1) + jnp.roll(source, -2, axis=1))
    laplace = along_x + transverse(source, GZ)
    atom_count = selector.shape[0]
    orbital_count = source.shape[0]
    blocks = jnp.einsum('ajx,nxp->anjp', selector, source, precision=highest)
    blocks = blocks.reshape(atom_count, orbital_count, BPTS)
    coupled = jnp.einsum('anq,aqf->anf', blocks, atom_tables, precision=highest) * atom_coef[:, None, :]
    spread_back = jnp.einsum('anf,aqf->anq', coupled, atom_tables, precision=highest)
    spread_back = spread_back.reshape(atom_count, orbital_count, BP, GY * GZ)
    nonlocal_part = jnp.einsum('ajx,anjp->nxp', selector, spread_back, precision=highest)
    return -0.5 * laplace + potential[None] * source + nonlocal_part

def chebyshev(start, hamiltonian_fn, cut_value, top_value):
    half_width = (top_value - cut_value) / 2.0
    centre = (top_value + cut_value) / 2.0
    sigma_now = half_width / (low_edge - centre)
    tau_value = 2.0 / sigma_now
    previous = start
    current = (hamiltonian_fn(previous) - centre * previous) * (sigma_now / half_width)
    for step_index in range(ORDER - 1):
        sigma_next = 1.0 / (tau_value - sigma_now)
        upcoming = (hamiltonian_fn(current) - centre * current) * (2.0 * sigma_next / half_width) - sigma_now * sigma_next * previous
        previous = current
        current = upcoming
        sigma_now = sigma_next
    return current

def reference(orbitals, potential, projectors, atom_kind, atom_plane, atom_coef, filter_cut, filter_top):
    plane_ids = jnp.arange(GX).astype(jnp.int32)
    depth_ids = jnp.arange(BP).astype(jnp.int32)
    selector = (plane_ids[None, None, :] == atom_plane.astype(jnp.int32)[:, None, None] + depth_ids[None, :, None]).astype(jnp.float32)
    atom_tables = projectors[atom_kind]
    cut_value = filter_cut[0]
    top_value = filter_top[0]

    def hamiltonian_fn(source):
        return hamiltonian(source, potential, selector, atom_tables, atom_coef)
    group_size = 32 if NB % 32 == 0 else NB
    groups = orbitals.reshape(NB // group_size, group_size, GX, GY * GZ)
    filtered = lax.map(lambda group_block: chebyshev(group_block, hamiltonian_fn, cut_value, top_value), groups)
    filtered = filtered.reshape(NB, NPTS)
    gram_matrix = jnp.dot(filtered, filtered.T, precision=highest) / NPTS
    factor = jnp.linalg.cholesky(gram_matrix)
    return jax.scipy.linalg.solve_triangular(factor, filtered, lower=True)
```

```python
import functools
import jax
import jax.numpy as jnp
from jax import lax
from jax.experimental import pallas as pl
from jax.experimental.pallas import tpu as pltpu
from jax.sharding import PartitionSpec as P

GZ = 32
ORDER = 6

low_edge = -1.0
highest = lax.Precision.HIGHEST
f32 = jnp.float32
bf16 = jnp.bfloat16
MESH = pl.DeviceIdType.MESH


def halves(value):
    high = value.astype(bf16)
    return high, (value - high.astype(f32)).astype(bf16)


def chebyshev_scalars(cut, top):
    half = (top - cut) / 2.0
    centre = (top + cut) / 2.0
    sigma = half / (low_edge - centre)
    tau = 2.0 / sigma
    pairs = [(sigma / half, None)]
    for _ in range(ORDER - 1):
        following = 1.0 / (tau - sigma)
        pairs.append((2.0 * following / half, sigma * following))
        sigma = following
    return centre, pairs


def filter_kernel(
    groups, plane_ref, kind_ref, scal_ref, orb_ref, pot_ref, coef_ref, proj_ref,
    out_ref, table, back, lap, even, odd, split, spread, halo, raw, load_sem, table_sem, own_sem,
    send_sem, recv_sem, out_sem, in_sem,
):
    rows, planes, points = orb_ref.shape
    kinds, block, funcs = proj_ref.shape
    atoms = coef_ref.shape[0]
    depth = block // points
    share = rows // groups
    width = out_ref.shape[2]
    slabs, bands = lax.axis_size("slab"), lax.axis_size("band")
    me, my_band = lax.axis_index("slab"), lax.axis_index("band")
    right, left = lax.rem(me + 1, slabs), lax.rem(me + slabs - 1, slabs)

    loads = []
    for x in range(planes):
        loads.append(pltpu.make_async_copy(orb_ref.at[:, x], even.at[x], load_sem.at[x]))
        loads[-1].start()
    tables = []
    for k in range(kinds):
        tables.append(pltpu.make_async_copy(proj_ref.at[k], raw.at[k], table_sem.at[k]))
        tables[-1].start()

    barrier = pltpu.get_barrier_semaphore()
    for neighbour in (left, right):
        pl.semaphore_signal(barrier, inc=1, device_id={"slab": neighbour}, device_id_type=MESH)
    for d in range(1, bands):
        pl.semaphore_signal(barrier, inc=1, device_id={"band": lax.rem(my_band + d, bands)}, device_id_type=MESH)
    pl.semaphore_wait(barrier, bands + 1)

    zeros = jnp.zeros((rows, points), f32)

    def clear(x, c):
        odd[x] = zeros
        return c

    lax.fori_loop(0, planes, clear, 0)

    def clear_spread(a, c):
        spread[a, 0] = zeros[:share]
        spread[a, depth + 1] = zeros[:share]
        return c

    lax.fori_loop(0, atoms, clear_spread, 0)

    strip = 64

    def lap_rows(i, c):
        r = lax.broadcasted_iota(jnp.int32, (strip, points), 0) + i * strip
        q = lax.broadcasted_iota(jnp.int32, (strip, points), 1)
        dy = jnp.abs(r // GZ - q // GZ)
        dz = jnp.abs(r % GZ - q % GZ)

        def line(d):
            return jnp.where(d == 0, -30.0, jnp.where(d == 1, 16.0, jnp.where(d == 2, -1.0, 0.0)))

        lap[pl.ds(i * strip, strip)] = (jnp.where(dz == 0, line(dy), 0.0) + jnp.where(dy == 0, line(dz), 0.0)).astype(bf16)
        return c

    lax.fori_loop(0, points // strip, lap_rows, 0)

    part = 256

    for k in range(kinds):
        tables[k].wait()

        def convert(i, c):
            at = pl.ds(i * part, part)
            high, low = halves(raw[k, at])
            table[k, at, :funcs] = high
            table[k, at, funcs:] = low
            lanes = pl.ds(pl.multiple_of(i * part, part), part)
            back[k, :funcs, lanes] = high.T
            back[k, funcs:, lanes] = low.T
            return c

        lax.fori_loop(0, block // part, convert, 0)

    for copy in loads:
        copy.wait()

    centre = scal_ref[2 * ORDER]
    quad = 4
    places = [plane_ref[a] - me * planes for a in range(atoms)]
    order = sorted(range(1, bands), key=lambda d: abs(d - bands / 2))
    unit = min(width, points)
    units = width // unit

    def outgoing(g, d, u):
        rs = pl.ds(pl.multiple_of(g * share, share), share)
        target = lax.rem(my_band + d, bands)
        if width >= points:
            src = even.at[target * units + u, rs]
        else:
            per = points // width
            src = even.at[target // per, rs, pl.ds(pl.multiple_of(lax.rem(target, per) * width, 128), width)]
        return pltpu.make_async_remote_copy(
            src_ref=src,
            dst_ref=out_ref.at[my_band, rs, u * unit : (u + 1) * unit],
            send_sem=out_sem.at[g, d - 1, u],
            recv_sem=in_sem.at[g, d - 1, u],
            device_id={"band": target},
            device_id_type=MESH,
        )

    def own(u):
        if width >= points:
            src = even.at[my_band * units + u]
        else:
            per = points // width
            src = even.at[my_band // per, :, pl.ds(pl.multiple_of(lax.rem(my_band, per) * width, 128), width)]
        return pltpu.make_async_copy(src, out_ref.at[my_band, :, u * unit : (u + 1) * unit], own_sem.at[u])

    def group_step(g, first):
        rs = pl.ds(first, share)

        def split_plane(x, c):
            high, low = halves(even[x, rs])
            split[x, :share] = high
            split[x, share:] = low
            return c

        lax.fori_loop(0, planes, split_plane, 0)

        def step(s, cur, nxt):
            scale = scal_ref[2 * s]
            pull = scal_ref[2 * s + 1]
            copies = []
            for side, start, target in ((0, planes - 2, right), (1, 0, left)):
                copy = pltpu.make_async_remote_copy(
                    src_ref=cur.at[pl.ds(start, 2), rs],
                    dst_ref=halo.at[g, s, side],
                    send_sem=send_sem.at[side],
                    recv_sem=recv_sem.at[g, s, side],
                    device_id={"slab": target},
                    device_id_type=MESH,
                )
                copy.start()
                copies.append(copy)

            def atom(a, c):
                p = jnp.clip(plane_ref[a] - me * planes, 0, planes - depth)
                k = kind_ref[a]
                both = jnp.concatenate([split[p + j] for j in range(depth)], axis=1)
                r = jnp.dot(both, table[k], preferred_element_type=f32)
                coupled = r[:share, :funcs] + (r[:share, funcs:] + r[share:, :funcs])
                high, low = halves(coupled * coef_ref[pl.ds(a, 1)])
                pair = jnp.concatenate(
                    [jnp.concatenate([high, high], axis=1), jnp.concatenate([low, low], axis=1)], axis=0
                )
                for j in range(depth):
                    r = jnp.dot(pair, back[k, :, j * points : (j + 1) * points], preferred_element_type=f32)
                    spread[a, j + 1] = r[:share] + r[share:]
                return c

            lax.fori_loop(0, atoms, atom, 0, unroll=True)

            slots = {x: [jnp.clip(x - places[a], -1, depth) + 1 for a in range(atoms)] for x in range(planes)}

            def quads(xs, take):
                both = jnp.concatenate([split[x] for x in xs], axis=0)
                r = jnp.dot(both, lap[...], preferred_element_type=f32)
                piece = min(16, share)
                span = min(256, points)
                for r0, l0 in [(r0, l0) for r0 in range(0, share, piece) for l0 in range(0, points, span)]:
                    ls = slice(l0, l0 + span)
                    fs = {}
                    for x in xs:
                        for d in (-2, -1, 0, 1, 2):
                            if x + d not in fs:
                                fs[x + d] = take(x + d, r0, piece, ls)
                    for i, x in enumerate(xs):
                        base = i * 2 * share + r0
                        total = (r[base : base + piece, ls] + r[base + share : base + share + piece, ls]) * (-0.5 / 12.0)
                        total = total + (pot_ref[pl.ds(x, 1), ls] + (1.25 - centre)) * fs[x]
                        total = total + (fs[x - 1] + fs[x + 1]) * (-2.0 / 3.0) + (fs[x - 2] + fs[x + 2]) * (1.0 / 24.0)
                        for a in range(atoms):
                            total = total + spread[a, slots[x][a], r0 : r0 + piece, ls]
                        at = (x, pl.ds(first + r0, piece), ls)
                        fresh = scale * total - pull * nxt[at]
                        nxt[at] = fresh
                        high, low = halves(fresh)
                        split[x, r0 : r0 + piece, ls] = high
                        split[x, share + r0 : share + r0 + piece, ls] = low

            def take(x, r0, piece, ls):
                if x < 0:
                    return halo[g, s, 0, x + 2, r0 : r0 + piece, ls]
                if x >= planes:
                    return halo[g, s, 1, x - planes, r0 : r0 + piece, ls]
                return cur[x, pl.ds(first + r0, piece), ls]

            for x0 in range(2, planes - 2, quad):
                quads(list(range(x0, min(x0 + quad, planes - 2))), take)
            for copy in copies:
                copy.wait()
            quads([0, 1, planes - 2, planes - 1], take)

        def two(i, c):
            step(2 * i, even, odd)
            step(2 * i + 1, odd, even)
            return c

        lax.fori_loop(0, ORDER // 2, two, 0)

    def run_group(g, c):
        group_step(g, pl.multiple_of(g * share, share))
        for d in order:
            for u in range(units):
                outgoing(g, d, u).start()
        return c

    lax.fori_loop(0, groups, run_group, 0)
    for u in range(units):
        own(u).start()
    for g in range(groups):
        for d in order:
            for u in range(units):
                outgoing(g, d, u).wait()
    for u in range(units):
        own(u).wait()


def filter_call(plane, kind, scal, orb, pot, coef, proj, groups):
    rows, planes, points = orb.shape
    atoms = coef.shape[0]
    kinds, block, funcs = proj.shape
    depth = block // points
    bands = lax.axis_size("band")
    share = rows // groups
    width = planes * points // bands
    units = max(width // points, 1)
    smem = pl.BlockSpec(memory_space=pltpu.SMEM)
    vmem = pl.BlockSpec(memory_space=pltpu.VMEM)
    hbm = pl.BlockSpec(memory_space=pl.ANY)
    dma = pltpu.SemaphoreType.DMA
    return pl.pallas_call(
        functools.partial(filter_kernel, groups),
        out_shape=jax.ShapeDtypeStruct((bands, rows, planes * points // bands), f32),
        in_specs=[smem] * 3 + [hbm, vmem, vmem, hbm],
        out_specs=vmem,
        scratch_shapes=[
            pltpu.VMEM((kinds, block, 2 * funcs), bf16),
            pltpu.VMEM((kinds, 2 * funcs, block), bf16),
            pltpu.VMEM((points, points), bf16),
            pltpu.VMEM((planes, rows, points), f32),
            pltpu.VMEM((planes, rows, points), f32),
            pltpu.VMEM((planes, 2 * share, points), bf16),
            pltpu.VMEM((atoms, depth + 2, share, points), f32),
            pltpu.VMEM((groups, ORDER, 2, 2, share, points), f32),
            pltpu.VMEM((kinds, block, funcs), f32),
            dma((planes,)),
            dma((kinds,)),
            dma((units,)),
            dma((2,)),
            dma((groups, ORDER, 2)),
            dma((groups, bands - 1, units)),
            dma((groups, bands - 1, units)),
        ],
        compiler_params=pltpu.CompilerParams(
            collective_id=0, has_side_effects=True, vmem_limit_bytes=60 * 1024 * 1024
        ),
        name="cheb_filter",
    )(plane, kind, scal, orb, pot, coef, proj)


def factor_kernel(nb, g_ref, w_ref, a_ref, d_ref):
    n = w_ref.shape[0]
    a_ref[...] = jnp.zeros((n, n), f32)
    at = 0
    for i in range(n // nb):
        for j in range(i + 1):
            a_ref[i * nb : (i + 1) * nb, j * nb : (j + 1) * nb] = g_ref[at : at + nb]
            at += nb
    w_ref[...] = jnp.zeros((n, n), f32)
    rows = lax.broadcasted_iota(jnp.int32, (nb, nb), 0)
    cols = lax.broadcasted_iota(jnp.int32, (nb, nb), 1)
    row_ids = lax.broadcasted_iota(jnp.int32, (nb, 1), 0)
    lane_ids = lax.broadcasted_iota(jnp.int32, (1, nb), 1)
    nt = (((1,), (1,)), ((), ()))
    for b in range(n // nb):
        lo, hi = b * nb, (b + 1) * nb
        d_ref[:, :nb] = a_ref[lo:hi, lo:hi]
        d_ref[:, nb:] = (rows == cols).astype(f32)

        def eliminate(t, c):
            k = 2 * t
            top = d_ref[pl.ds(k, 1), :]
            low = d_ref[pl.ds(k + 1, 1), :]
            block = d_ref[:, :nb]

            def lane(row, at):
                return jnp.sum(jnp.where(lane_ids == at, row[:, :nb], 0.0), axis=1, keepdims=True)

            def column(at):
                return jnp.sum(jnp.where(cols == at, block, 0.0), axis=1, keepdims=True)

            p11, p12, p22 = lane(top, k), lane(top, k + 1), lane(low, k + 1)
            c0, c1 = column(k), column(k + 1)
            inv1 = 1.0 / p11
            link = p12 * inv1
            inv2 = 1.0 / (p22 - p12 * link)
            low = (low - link * top) * inv2
            c1 = jnp.where(row_ids > k + 1, c1 - link * c0, 0.0)
            c0 = jnp.where(row_ids > k, c0, 0.0)
            d_ref[...] = d_ref[...] - c0 * (top * inv1) - c1 * low
            return c

        lax.fori_loop(0, nb // 2, eliminate, 0)
        pivots = jnp.sum(jnp.where(rows == cols, d_ref[:, :nb], 0.0), axis=1, keepdims=True)
        inverse = d_ref[:, nb:] / jnp.sqrt(pivots)
        w_ref[lo:hi, lo:hi] = inverse
        if lo > 0:
            mixed = jnp.dot(a_ref[lo:hi, :lo], w_ref[:lo, :lo], precision=highest, preferred_element_type=f32)
            w_ref[lo:hi, :lo] = -jnp.dot(inverse, mixed, precision=highest, preferred_element_type=f32)
        if hi < n:
            panel = lax.dot_general(a_ref[hi:, lo:hi], inverse, nt, precision=highest, preferred_element_type=f32)
            a_ref[hi:, lo:hi] = panel
            a_ref[hi:, hi:] = a_ref[hi:, hi:] - lax.dot_general(
                panel, panel, nt, precision=highest, preferred_element_type=f32
            )


def inverse_factor(blocks, n):
    nb = block_size(n)
    vmem = pl.BlockSpec(memory_space=pltpu.VMEM)
    return pl.pallas_call(
        functools.partial(factor_kernel, nb),
        out_shape=jax.ShapeDtypeStruct((n, n), f32),
        in_specs=[vmem],
        out_specs=vmem,
        scratch_shapes=[pltpu.VMEM((n, n), f32), pltpu.VMEM((nb, 2 * nb), f32)],
        compiler_params=pltpu.CompilerParams(vmem_limit_bytes=32 * 1024 * 1024),
        name="factor_inverse",
    )(blocks)


def reduce_kernel(nb, g_ref, out_ref, pack, first, part, second, full, sends, recvs_a, recvs_b, recvs_c, recvs_d):
    n = g_ref.shape[0]
    total = pack.shape[0]
    slabs, bands = lax.axis_size("slab"), lax.axis_size("band")
    my_slab, my_band = lax.axis_index("slab"), lax.axis_index("band")
    deep, thin = total // slabs, total // slabs // bands
    at = 0
    for i in range(n // nb):
        for j in range(i + 1):
            pack[at : at + nb] = g_ref[i * nb : (i + 1) * nb, j * nb : (j + 1) * nb]
            at += nb
    if at < total:
        pack[at:] = jnp.zeros((total - at, nb), f32)

    def peer(me, size, d):
        return lax.rem(me + d, size)

    barrier = pltpu.get_barrier_semaphore()
    for axis, me, size in (("slab", my_slab, slabs), ("band", my_band, bands)):
        for d in range(1, size):
            pl.semaphore_signal(
                barrier, inc=1, device_id={axis: peer(me, size, d)}, device_id_type=pl.DeviceIdType.MESH
            )
    pl.semaphore_wait(barrier, slabs + bands - 2)

    def exchange(axis, me, size, source, target, recvs):
        copies = []
        for d in range(1, size):
            other = peer(me, size, d)
            copies.append(
                pltpu.make_async_remote_copy(
                    src_ref=source(other),
                    dst_ref=target(d),
                    send_sem=sends.at[d - 1],
                    recv_sem=recvs.at[d - 1],
                    device_id={axis: other},
                    device_id_type=pl.DeviceIdType.MESH,
                )
            )
        for copy in copies:
            copy.start()
        for copy in copies:
            copy.wait()

    def span(start, length):
        return pl.ds(pl.multiple_of(start, 8), length)

    exchange(
        "slab", my_slab, slabs, lambda t: pack.at[span(t * deep, deep)], lambda d: first.at[d - 1], recvs_a
    )
    value = pack[span(my_slab * deep, deep)]
    for d in range(1, slabs):
        value = value + first[d - 1]
    part[...] = value
    exchange(
        "band", my_band, bands, lambda t: part.at[span(t * thin, thin)], lambda d: second.at[d - 1], recvs_b
    )
    value = part[span(my_band * thin, thin)]
    for d in range(1, bands):
        value = value + second[d - 1]
    mine = span(my_slab * deep + my_band * thin, thin)
    full[mine] = value
    exchange("band", my_band, bands, lambda t: full.at[mine], lambda d: full.at[mine], recvs_c)
    mine_deep = span(my_slab * deep, deep)
    exchange("slab", my_slab, slabs, lambda t: full.at[mine_deep], lambda d: full.at[mine_deep], recvs_d)
    out_ref[...] = full[...]


def block_size(n):
    return 128 if n % 128 == 0 else n


def reduced_blocks(gram):
    n = gram.shape[0]
    nb = block_size(n)
    slabs, bands = lax.axis_size("slab"), lax.axis_size("band")
    count = n // nb
    used = count * (count + 1) // 2 * nb
    unit = 8 * slabs * bands
    total = (used + unit - 1) // unit * unit
    vmem = pl.BlockSpec(memory_space=pltpu.VMEM)
    dma = pltpu.SemaphoreType.DMA
    return pl.pallas_call(
        functools.partial(reduce_kernel, nb),
        out_shape=jax.ShapeDtypeStruct((total, nb), f32),
        in_specs=[vmem],
        out_specs=vmem,
        scratch_shapes=[
            pltpu.VMEM((total, nb), f32),
            pltpu.VMEM((slabs - 1, total // slabs, nb), f32),
            pltpu.VMEM((total // slabs, nb), f32),
            pltpu.VMEM((bands - 1, total // slabs // bands, nb), f32),
            pltpu.VMEM((total, nb), f32),
            dma((max(slabs, bands) - 1,)),
            dma((slabs - 1,)),
            dma((bands - 1,)),
            dma((bands - 1,)),
            dma((slabs - 1,)),
        ],
        compiler_params=pltpu.CompilerParams(
            collective_id=1, has_side_effects=True, vmem_limit_bytes=32 * 1024 * 1024
        ),
        name="gram_sum",
    )(gram)


def local(
    orbitals, potential, projectors, atom_kind, atom_plane, atom_coef, filter_cut, filter_top
):
    rows = orbitals.shape[0]
    centre, pairs = chebyshev_scalars(filter_cut[0], filter_top[0])
    scal = []
    for a, b in pairs:
        scal += [a, jnp.zeros((), f32) if b is None else b]
    scal = jnp.stack(scal + [centre])
    filtered = filter_call(
        atom_plane, atom_kind, scal, orbitals, potential, atom_coef, projectors, 2 if rows % 32 == 0 else 1
    )
    grid_layout = filtered.reshape(-1, filtered.shape[2])
    point_total = grid_layout.shape[1] * lax.axis_size(("band", "slab"))
    gram = jnp.dot(grid_layout, grid_layout.T, precision=highest) / point_total
    factor_inverse = inverse_factor(reduced_blocks(gram), gram.shape[0])
    return jnp.dot(factor_inverse, grid_layout, precision=lax.Precision.HIGH)


def solution(mesh):
    in_specs = (
        P("band", "slab", None),
        P("slab", None),
        P(),
        P("slab"),
        P("slab"),
        P("slab", None),
        P(),
        P(),
    )
    out_specs = P(None, ("slab", "band"))
    return jax.shard_map(local, mesh=mesh, in_specs=in_specs, out_specs=out_specs, check_vma=False)
```

```python
import functools
import jax
import jax.numpy as jnp
from jax import lax
from jax.experimental import pallas as pl
from jax.experimental.pallas import tpu as pltpu
from jax.sharding import PartitionSpec as P

GZ = 32
ORDER = 6

low_edge = -1.0
highest = lax.Precision.HIGHEST
f32 = jnp.float32
bf16 = jnp.bfloat16
MESH = pl.DeviceIdType.MESH


def halves(value):
    high = value.astype(bf16)
    return high, (value - high.astype(f32)).astype(bf16)


def chebyshev_scalars(cut, top):
    half = (top - cut) / 2.0
    centre = (top + cut) / 2.0
    sigma = half / (low_edge - centre)
    tau = 2.0 / sigma
    pairs = [(sigma / half, None)]
    for _ in range(ORDER - 1):
        following = 1.0 / (tau - sigma)
        pairs.append((2.0 * following / half, sigma * following))
        sigma = following
    return centre, pairs


def pair_slots(atoms, kinds):
    return min(atoms, (atoms + kinds) // 2)


def filter_kernel(
    groups, plane_ref, kind_ref, scal_ref, orb_ref, pot_ref, coef_ref, proj_ref,
    out_ref, table, back, lap, even, odd, split, spread, halo, raw, pairs, load_sem, table_sem, own_sem,
    send_sem, recv_sem, out_sem, in_sem,
):
    rows, planes, points = orb_ref.shape
    kinds, block, funcs = proj_ref.shape
    atoms = coef_ref.shape[0]
    depth = block // points
    share = rows // groups
    width = out_ref.shape[2]
    slabs, bands = lax.axis_size("slab"), lax.axis_size("band")
    me, my_band = lax.axis_index("slab"), lax.axis_index("band")
    right, left = lax.rem(me + 1, slabs), lax.rem(me + slabs - 1, slabs)

    loads = []
    for x in range(planes):
        loads.append(pltpu.make_async_copy(orb_ref.at[:, x], even.at[x], load_sem.at[x]))
        loads[-1].start()
    tables = []
    for k in range(kinds):
        tables.append(pltpu.make_async_copy(proj_ref.at[k], raw.at[k], table_sem.at[k]))
        tables[-1].start()

    barrier = pltpu.get_barrier_semaphore()
    for neighbour in (left, right):
        pl.semaphore_signal(barrier, inc=1, device_id={"slab": neighbour}, device_id_type=MESH)
    for d in range(1, bands):
        pl.semaphore_signal(barrier, inc=1, device_id={"band": lax.rem(my_band + d, bands)}, device_id_type=MESH)
    pl.semaphore_wait(barrier, bands + 1)

    zeros = jnp.zeros((rows, points), f32)

    def clear(x, c):
        odd[x] = zeros
        return c

    lax.fori_loop(0, planes, clear, 0)

    def clear_spread(a, c):
        spread[a, 0] = zeros[:share]
        spread[a, depth + 1] = zeros[:share]
        return c

    lax.fori_loop(0, spread.shape[0], clear_spread, 0)

    strip = 64

    def lap_rows(i, c):
        r = lax.broadcasted_iota(jnp.int32, (strip, points), 0) + i * strip
        q = lax.broadcasted_iota(jnp.int32, (strip, points), 1)
        dy = jnp.abs(r // GZ - q // GZ)
        dz = jnp.abs(r % GZ - q % GZ)

        def line(d):
            return jnp.where(d == 0, -30.0, jnp.where(d == 1, 16.0, jnp.where(d == 2, -1.0, 0.0)))

        lap[pl.ds(i * strip, strip)] = (jnp.where(dz == 0, line(dy), 0.0) + jnp.where(dy == 0, line(dz), 0.0)).astype(bf16)
        return c

    lax.fori_loop(0, points // strip, lap_rows, 0)

    part = 256

    for k in range(kinds):
        tables[k].wait()

        def convert(i, c):
            at = pl.ds(i * part, part)
            high, low = halves(raw[k, at])
            table[k, at, :funcs] = high
            table[k, at, funcs:] = low
            lanes = pl.ds(pl.multiple_of(i * part, part), part)
            back[k, :funcs, lanes] = high.T
            back[k, funcs:, lanes] = low.T
            return c

        lax.fori_loop(0, block // part, convert, 0)

    for copy in loads:
        copy.wait()

    slot_count = pair_slots(atoms, kinds)
    kind_of = [jnp.clip(kind_ref[a], 0, kinds - 1) for a in range(atoms)]
    base, bases = 0, []
    for k in range(kinds):
        bases.append(base)
        base = base + (sum((kind_of[a] == k).astype(jnp.int32) for a in range(atoms)) + 1) // 2
    seats = []
    for a in range(atoms):
        rank = sum(((kind_of[b] == kind_of[a]).astype(jnp.int32) for b in range(a)), jnp.int32(0))
        start = sum(jnp.where(kind_of[a] == k, bases[k], 0) for k in range(kinds))
        seats.append(2 * start + rank)
        pairs[0, a] = seats[a]
    for seat in range(2 * slot_count):
        holder = sum(jnp.where(seats[a] == seat, a + 1, 0) for a in range(atoms))
        pairs[1, seat] = holder
    zero_row = jnp.zeros((1, funcs), f32)
    half = 16 if share % 16 == 0 else share

    def copies_from(source, g, s, piece):
        found = []
        for h in range(share // half) if piece is None else (piece,):
            rs = pl.ds(pl.multiple_of(g * share + h * half, 8), half)
            for side, start, target in ((0, planes - 2, right), (1, 0, left)):
                found.append(
                    pltpu.make_async_remote_copy(
                        src_ref=source.at[pl.ds(start, 2), rs],
                        dst_ref=halo.at[g, s, side, h],
                        send_sem=send_sem.at[g, side, h],
                        recv_sem=recv_sem.at[g, s, side, h],
                        device_id={"slab": target},
                        device_id_type=MESH,
                    )
                )
        return found

    for g in range(groups):
        for copy in copies_from(even, g, 0, None):
            copy.start()

    centre = scal_ref[2 * ORDER]
    quad = 4
    places = [plane_ref[a] - me * planes for a in range(atoms)]
    order = sorted(range(1, bands), key=lambda d: abs(d - bands / 2))
    unit = min(width, points)
    units = width // unit

    def outgoing(g, d, u):
        rs = pl.ds(pl.multiple_of(g * share, share), share)
        target = lax.rem(my_band + d, bands)
        if width >= points:
            src = even.at[target * units + u, rs]
        else:
            per = points // width
            src = even.at[target // per, rs, pl.ds(pl.multiple_of(lax.rem(target, per) * width, 128), width)]
        return pltpu.make_async_remote_copy(
            src_ref=src,
            dst_ref=out_ref.at[my_band, rs, u * unit : (u + 1) * unit],
            send_sem=out_sem.at[g, d - 1, u],
            recv_sem=in_sem.at[g, d - 1, u],
            device_id={"band": target},
            device_id_type=MESH,
        )

    def own(u):
        if width >= points:
            src = even.at[my_band * units + u]
        else:
            per = points // width
            src = even.at[my_band // per, :, pl.ds(pl.multiple_of(lax.rem(my_band, per) * width, 128), width)]
        return pltpu.make_async_copy(src, out_ref.at[my_band, :, u * unit : (u + 1) * unit], own_sem.at[u])

    def group_step(g, first):
        rs = pl.ds(first, share)

        def split_plane(x, c):
            high, low = halves(even[x, rs])
            split[x, :share] = high
            split[x, share:] = low
            return c

        lax.fori_loop(0, planes, split_plane, 0)

        def step(s, cur, nxt):
            scale = scal_ref[2 * s]
            pull = scal_ref[2 * s + 1]
            def pair(q, c):
                holders = [pairs[1, 2 * q + m] for m in range(2)]
                atom = [jnp.maximum(holder - 1, 0) for holder in holders]
                k = jnp.clip(kind_ref[atom[0]], 0, kinds - 1)
                places = [jnp.clip(plane_ref[atom[m]] - me * planes, 0, planes - depth) for m in range(2)]
                both = jnp.concatenate(
                    [jnp.concatenate([split[p + j] for j in range(depth)], axis=1) for p in places], axis=0
                )
                r = jnp.dot(both, table[k], preferred_element_type=f32)
                stack = []
                for m in range(2):
                    at = m * 2 * share
                    coupled = r[at : at + share, :funcs] + (
                        r[at : at + share, funcs:] + r[at + share : at + 2 * share, :funcs]
                    )
                    coef = jnp.where(holders[m] > 0, coef_ref[pl.ds(atom[m], 1)], zero_row)
                    for value in halves(coupled * coef):
                        stack.append(jnp.concatenate([value, value], axis=1))
                stack = jnp.concatenate(stack, axis=0)
                for j in range(depth):
                    r = jnp.dot(stack, back[k, :, j * points : (j + 1) * points], preferred_element_type=f32)
                    for m in range(2):
                        at = m * 2 * share
                        spread[2 * q + m, j + 1] = r[at : at + share] + r[at + share : at + 2 * share]
                return c

            lax.fori_loop(0, slot_count, pair, 0, unroll=True)

            seat_of = [pairs[0, a] for a in range(atoms)]
            slots = {x: [jnp.clip(x - places[a], -1, depth) + 1 for a in range(atoms)] for x in range(planes)}

            def quads(xs, take, before=None, after=None):
                both = jnp.concatenate([split[x] for x in xs], axis=0)
                r = jnp.dot(both, lap[...], preferred_element_type=f32)
                piece = min(16, share)
                span = min(256, points)
                for r0, l0 in [(r0, l0) for r0 in range(0, share, piece) for l0 in range(0, points, span)]:
                    ls = slice(l0, l0 + span)
                    if before is not None and r0 % half == 0 and l0 == 0:
                        before(r0 // half)
                    fs = {}
                    for x in xs:
                        for d in (-2, -1, 0, 1, 2):
                            if x + d not in fs:
                                fs[x + d] = take(x + d, r0, piece, ls)
                    for i, x in enumerate(xs):
                        base = i * 2 * share + r0
                        total = (r[base : base + piece, ls] + r[base + share : base + share + piece, ls]) * (-0.5 / 12.0)
                        total = total + (pot_ref[pl.ds(x, 1), ls] + (1.25 - centre)) * fs[x]
                        total = total + (fs[x - 1] + fs[x + 1]) * (-2.0 / 3.0) + (fs[x - 2] + fs[x + 2]) * (1.0 / 24.0)
                        for a in range(atoms):
                            total = total + spread[seat_of[a], slots[x][a], r0 : r0 + piece, ls]
                        at = (x, pl.ds(first + r0, piece), ls)
                        fresh = scale * total - pull * nxt[at]
                        nxt[at] = fresh
                        high, low = halves(fresh)
                        split[x, r0 : r0 + piece, ls] = high
                        split[x, share + r0 : share + r0 + piece, ls] = low
                    if after is not None and (r0 + piece) % half == 0 and l0 + span == points:
                        after(r0 // half)

            def take(x, r0, piece, ls):
                if x < 0:
                    return halo[g, s, 0, r0 // half, x + 2, r0 % half : r0 % half + piece, ls]
                if x >= planes:
                    return halo[g, s, 1, r0 // half, x - planes, r0 % half : r0 % half + piece, ls]
                return cur[x, pl.ds(first + r0, piece), ls]

            for x0 in range(2, planes - 2, quad):
                quads(list(range(x0, min(x0 + quad, planes - 2))), take)

            def before(h):
                for copy in copies_from(cur, g, s, h):
                    copy.wait()

            def after(h):
                @pl.when(s + 1 < ORDER)
                def _():
                    for copy in copies_from(nxt, g, s + 1, h):
                        copy.start()

            quads([0, 1, planes - 2, planes - 1], take, before, after)

        def two(i, c):
            step(2 * i, even, odd)
            step(2 * i + 1, odd, even)
            return c

        lax.fori_loop(0, ORDER // 2, two, 0)

    def run_group(g, c):
        group_step(g, pl.multiple_of(g * share, share))
        for d in order:
            for u in range(units):
                outgoing(g, d, u).start()
        return c

    lax.fori_loop(0, groups, run_group, 0)
    for u in range(units):
        own(u).start()
    for g in range(groups):
        for d in order:
            for u in range(units):
                outgoing(g, d, u).wait()
    for u in range(units):
        own(u).wait()


def filter_call(plane, kind, scal, orb, pot, coef, proj, groups):
    rows, planes, points = orb.shape
    atoms = coef.shape[0]
    kinds, block, funcs = proj.shape
    depth = block // points
    bands = lax.axis_size("band")
    share = rows // groups
    width = planes * points // bands
    units = max(width // points, 1)
    half = 16 if share % 16 == 0 else share
    smem = pl.BlockSpec(memory_space=pltpu.SMEM)
    vmem = pl.BlockSpec(memory_space=pltpu.VMEM)
    hbm = pl.BlockSpec(memory_space=pl.ANY)
    dma = pltpu.SemaphoreType.DMA
    return pl.pallas_call(
        functools.partial(filter_kernel, groups),
        out_shape=jax.ShapeDtypeStruct((bands, rows, planes * points // bands), f32),
        in_specs=[smem] * 3 + [hbm, vmem, vmem, hbm],
        out_specs=vmem,
        scratch_shapes=[
            pltpu.VMEM((kinds, block, 2 * funcs), bf16),
            pltpu.VMEM((kinds, 2 * funcs, block), bf16),
            pltpu.VMEM((points, points), bf16),
            pltpu.VMEM((planes, rows, points), f32),
            pltpu.VMEM((planes, rows, points), f32),
            pltpu.VMEM((planes, 2 * share, points), bf16),
            pltpu.VMEM((2 * pair_slots(atoms, kinds), depth + 2, share, points), f32),
            pltpu.VMEM((groups, ORDER, 2, share // half, 2, half, points), f32),
            pltpu.VMEM((kinds, block, funcs), f32),
            pltpu.SMEM((2, max(atoms, 2 * pair_slots(atoms, kinds))), jnp.int32),
            dma((planes,)),
            dma((kinds,)),
            dma((units,)),
            dma((groups, 2, share // half)),
            dma((groups, ORDER, 2, share // half)),
            dma((groups, bands - 1, units)),
            dma((groups, bands - 1, units)),
        ],
        compiler_params=pltpu.CompilerParams(
            collective_id=0, has_side_effects=True, vmem_limit_bytes=60 * 1024 * 1024
        ),
        name="cheb_filter",
    )(plane, kind, scal, orb, pot, coef, proj)


def factor_kernel(nb, g_ref, w_ref, a_ref, d_ref):
    n = w_ref.shape[0]
    a_ref[...] = jnp.zeros((n, n), f32)
    at = 0
    for i in range(n // nb):
        for j in range(i + 1):
            a_ref[i * nb : (i + 1) * nb, j * nb : (j + 1) * nb] = g_ref[at : at + nb]
            at += nb
    w_ref[...] = jnp.zeros((n, n), f32)
    rows = lax.broadcasted_iota(jnp.int32, (nb, nb), 0)
    cols = lax.broadcasted_iota(jnp.int32, (nb, nb), 1)
    row_ids = lax.broadcasted_iota(jnp.int32, (nb, 1), 0)
    lane_ids = lax.broadcasted_iota(jnp.int32, (1, nb), 1)
    nt = (((1,), (1,)), ((), ()))
    for b in range(n // nb):
        lo, hi = b * nb, (b + 1) * nb
        d_ref[:, :nb] = a_ref[lo:hi, lo:hi]
        d_ref[:, nb:] = (rows == cols).astype(f32)

        def eliminate(t, c):
            k = 2 * t
            top = d_ref[pl.ds(k, 1), :]
            low = d_ref[pl.ds(k + 1, 1), :]
            block = d_ref[:, :nb]

            def lane(row, at):
                return jnp.sum(jnp.where(lane_ids == at, row[:, :nb], 0.0), axis=1, keepdims=True)

            def column(at):
                return jnp.sum(jnp.where(cols == at, block, 0.0), axis=1, keepdims=True)

            p11, p12, p22 = lane(top, k), lane(top, k + 1), lane(low, k + 1)
            c0, c1 = column(k), column(k + 1)
            inv1 = 1.0 / p11
            link = p12 * inv1
            inv2 = 1.0 / (p22 - p12 * link)
            low = (low - link * top) * inv2
            c1 = jnp.where(row_ids > k + 1, c1 - link * c0, 0.0)
            c0 = jnp.where(row_ids > k, c0, 0.0)
            d_ref[...] = d_ref[...] - c0 * (top * inv1) - c1 * low
            return c

        lax.fori_loop(0, nb // 2, eliminate, 0)
        pivots = jnp.sum(jnp.where(rows == cols, d_ref[:, :nb], 0.0), axis=1, keepdims=True)
        inverse = d_ref[:, nb:] / jnp.sqrt(pivots)
        w_ref[lo:hi, lo:hi] = inverse
        if lo > 0:
            mixed = jnp.dot(a_ref[lo:hi, :lo], w_ref[:lo, :lo], precision=highest, preferred_element_type=f32)
            w_ref[lo:hi, :lo] = -jnp.dot(inverse, mixed, precision=highest, preferred_element_type=f32)
        if hi < n:
            panel = lax.dot_general(a_ref[hi:, lo:hi], inverse, nt, precision=highest, preferred_element_type=f32)
            a_ref[hi:, lo:hi] = panel
            a_ref[hi:, hi:] = a_ref[hi:, hi:] - lax.dot_general(
                panel, panel, nt, precision=highest, preferred_element_type=f32
            )


def inverse_factor(blocks, n):
    nb = block_size(n)
    vmem = pl.BlockSpec(memory_space=pltpu.VMEM)
    return pl.pallas_call(
        functools.partial(factor_kernel, nb),
        out_shape=jax.ShapeDtypeStruct((n, n), f32),
        in_specs=[vmem],
        out_specs=vmem,
        scratch_shapes=[pltpu.VMEM((n, n), f32), pltpu.VMEM((nb, 2 * nb), f32)],
        compiler_params=pltpu.CompilerParams(vmem_limit_bytes=32 * 1024 * 1024),
        name="factor_inverse",
    )(blocks)


def reduce_kernel(nb, g_ref, out_ref, pack, first, part, second, full, sends, recvs_a, recvs_b, recvs_c, recvs_d):
    n = g_ref.shape[0]
    total = pack.shape[0]
    slabs, bands = lax.axis_size("slab"), lax.axis_size("band")
    my_slab, my_band = lax.axis_index("slab"), lax.axis_index("band")
    deep, thin = total // slabs, total // slabs // bands
    at = 0
    for i in range(n // nb):
        for j in range(i + 1):
            pack[at : at + nb] = g_ref[i * nb : (i + 1) * nb, j * nb : (j + 1) * nb]
            at += nb
    if at < total:
        pack[at:] = jnp.zeros((total - at, nb), f32)

    def peer(me, size, d):
        return lax.rem(me + d, size)

    barrier = pltpu.get_barrier_semaphore()
    for axis, me, size in (("slab", my_slab, slabs), ("band", my_band, bands)):
        for d in range(1, size):
            pl.semaphore_signal(
                barrier, inc=1, device_id={axis: peer(me, size, d)}, device_id_type=pl.DeviceIdType.MESH
            )
    pl.semaphore_wait(barrier, slabs + bands - 2)

    def exchange(axis, me, size, source, target, recvs):
        copies = []
        for d in range(1, size):
            other = peer(me, size, d)
            copies.append(
                pltpu.make_async_remote_copy(
                    src_ref=source(other),
                    dst_ref=target(d),
                    send_sem=sends.at[d - 1],
                    recv_sem=recvs.at[d - 1],
                    device_id={axis: other},
                    device_id_type=pl.DeviceIdType.MESH,
                )
            )
        for copy in copies:
            copy.start()
        for copy in copies:
            copy.wait()

    def span(start, length):
        return pl.ds(pl.multiple_of(start, 8), length)

    exchange(
        "slab", my_slab, slabs, lambda t: pack.at[span(t * deep, deep)], lambda d: first.at[d - 1], recvs_a
    )
    value = pack[span(my_slab * deep, deep)]
    for d in range(1, slabs):
        value = value + first[d - 1]
    part[...] = value
    exchange(
        "band", my_band, bands, lambda t: part.at[span(t * thin, thin)], lambda d: second.at[d - 1], recvs_b
    )
    value = part[span(my_band * thin, thin)]
    for d in range(1, bands):
        value = value + second[d - 1]
    mine = span(my_slab * deep + my_band * thin, thin)
    full[mine] = value
    exchange("band", my_band, bands, lambda t: full.at[mine], lambda d: full.at[mine], recvs_c)
    mine_deep = span(my_slab * deep, deep)
    exchange("slab", my_slab, slabs, lambda t: full.at[mine_deep], lambda d: full.at[mine_deep], recvs_d)
    out_ref[...] = full[...]


def block_size(n):
    return 128 if n % 128 == 0 else n


def reduced_blocks(gram):
    n = gram.shape[0]
    nb = block_size(n)
    slabs, bands = lax.axis_size("slab"), lax.axis_size("band")
    count = n // nb
    used = count * (count + 1) // 2 * nb
    unit = 8 * slabs * bands
    total = (used + unit - 1) // unit * unit
    vmem = pl.BlockSpec(memory_space=pltpu.VMEM)
    dma = pltpu.SemaphoreType.DMA
    return pl.pallas_call(
        functools.partial(reduce_kernel, nb),
        out_shape=jax.ShapeDtypeStruct((total, nb), f32),
        in_specs=[vmem],
        out_specs=vmem,
        scratch_shapes=[
            pltpu.VMEM((total, nb), f32),
            pltpu.VMEM((slabs - 1, total // slabs, nb), f32),
            pltpu.VMEM((total // slabs, nb), f32),
            pltpu.VMEM((bands - 1, total // slabs // bands, nb), f32),
            pltpu.VMEM((total, nb), f32),
            dma((max(slabs, bands) - 1,)),
            dma((slabs - 1,)),
            dma((bands - 1,)),
            dma((bands - 1,)),
            dma((slabs - 1,)),
        ],
        compiler_params=pltpu.CompilerParams(
            collective_id=1, has_side_effects=True, vmem_limit_bytes=32 * 1024 * 1024
        ),
        name="gram_sum",
    )(gram)


def local(
    orbitals, potential, projectors, atom_kind, atom_plane, atom_coef, filter_cut, filter_top
):
    rows = orbitals.shape[0]
    centre, pairs = chebyshev_scalars(filter_cut[0], filter_top[0])
    scal = []
    for a, b in pairs:
        scal += [a, jnp.zeros((), f32) if b is None else b]
    scal = jnp.stack(scal + [centre])
    filtered = filter_call(
        atom_plane, atom_kind, scal, orbitals, potential, atom_coef, projectors, 2 if rows % 32 == 0 else 1
    )
    grid_layout = filtered.reshape(-1, filtered.shape[2])
    point_total = grid_layout.shape[1] * lax.axis_size(("band", "slab"))
    gram = jnp.dot(grid_layout, grid_layout.T, precision=highest) / point_total
    factor_inverse = inverse_factor(reduced_blocks(gram), gram.shape[0])
    return jnp.dot(factor_inverse, grid_layout, precision=lax.Precision.HIGH)


def solution(mesh):
    in_specs = (
        P("band", "slab", None),
        P("slab", None),
        P(),
        P("slab"),
        P("slab"),
        P("slab", None),
        P(),
        P(),
    )
    out_specs = P(None, ("slab", "band"))
    return jax.shard_map(local, mesh=mesh, in_specs=in_specs, out_specs=out_specs, check_vma=False)
```

```python
import functools
import jax
import jax.numpy as jnp
from jax import lax
from jax.experimental import pallas as pl
from jax.experimental.pallas import tpu as pltpu
from jax.sharding import PartitionSpec as P

GZ = 32
ORDER = 6
micro = 8

low_edge = -1.0
highest = lax.Precision.HIGHEST
f32 = jnp.float32
bf16 = jnp.bfloat16
MESH = pl.DeviceIdType.MESH


def halves(value):
    high = value.astype(bf16)
    return high, (value - high.astype(f32)).astype(bf16)


def chebyshev_scalars(cut, top):
    half = (top - cut) / 2.0
    centre = (top + cut) / 2.0
    sigma = half / (low_edge - centre)
    tau = 2.0 / sigma
    pairs = [(sigma / half, None)]
    for _ in range(ORDER - 1):
        following = 1.0 / (tau - sigma)
        pairs.append((2.0 * following / half, sigma * following))
        sigma = following
    return centre, pairs


def pair_slots(atoms, kinds):
    return min(atoms, (atoms + kinds) // 2)


def filter_kernel(
    groups, plane_ref, kind_ref, scal_ref, orb_ref, pot_ref, coef_ref, proj_ref,
    out_ref, table, back, lap, even, odd, split, spread, halo, raw, pairs, load_sem, table_sem, own_sem,
    send_sem, recv_sem, out_sem, in_sem,
):
    rows, planes, points = orb_ref.shape
    kinds, block, funcs = proj_ref.shape
    atoms = coef_ref.shape[0]
    depth = block // points
    share = rows // groups
    width = out_ref.shape[2]
    slabs, bands = lax.axis_size("slab"), lax.axis_size("band")
    me, my_band = lax.axis_index("slab"), lax.axis_index("band")
    right, left = lax.rem(me + 1, slabs), lax.rem(me + slabs - 1, slabs)

    loads = []
    for x in range(planes):
        loads.append(pltpu.make_async_copy(orb_ref.at[:, x], even.at[x], load_sem.at[x]))
        loads[-1].start()
    tables = []
    for k in range(kinds):
        tables.append(pltpu.make_async_copy(proj_ref.at[k], raw.at[k], table_sem.at[k]))
        tables[-1].start()

    barrier = pltpu.get_barrier_semaphore()
    for neighbour in (left, right):
        pl.semaphore_signal(barrier, inc=1, device_id={"slab": neighbour}, device_id_type=MESH)
    for d in range(1, bands):
        pl.semaphore_signal(barrier, inc=1, device_id={"band": lax.rem(my_band + d, bands)}, device_id_type=MESH)
    pl.semaphore_wait(barrier, bands + 1)

    zeros = jnp.zeros((rows, points), f32)

    def clear(x, c):
        odd[x] = zeros
        return c

    lax.fori_loop(0, planes, clear, 0)

    def clear_spread(a, c):
        spread[a, 0] = zeros[:share]
        spread[a, depth + 1] = zeros[:share]
        return c

    lax.fori_loop(0, spread.shape[0], clear_spread, 0)

    strip = 64

    def lap_rows(i, c):
        r = lax.broadcasted_iota(jnp.int32, (strip, points), 0) + i * strip
        q = lax.broadcasted_iota(jnp.int32, (strip, points), 1)
        dy = jnp.abs(r // GZ - q // GZ)
        dz = jnp.abs(r % GZ - q % GZ)

        def line(d):
            return jnp.where(d == 0, -30.0, jnp.where(d == 1, 16.0, jnp.where(d == 2, -1.0, 0.0)))

        lap[pl.ds(i * strip, strip)] = (jnp.where(dz == 0, line(dy), 0.0) + jnp.where(dy == 0, line(dz), 0.0)).astype(bf16)
        return c

    lax.fori_loop(0, points // strip, lap_rows, 0)

    part = 256

    for k in range(kinds):
        tables[k].wait()

        def convert(i, c):
            at = pl.ds(i * part, part)
            high, low = halves(raw[k, at])
            table[k, at, :funcs] = high
            table[k, at, funcs:] = low
            lanes = pl.ds(pl.multiple_of(i * part, part), part)
            back[k, :funcs, lanes] = high.T
            back[k, funcs:, lanes] = low.T
            return c

        lax.fori_loop(0, block // part, convert, 0)

    for copy in loads:
        copy.wait()

    slot_count = pair_slots(atoms, kinds)
    kind_of = [jnp.clip(kind_ref[a], 0, kinds - 1) for a in range(atoms)]
    base, bases = 0, []
    for k in range(kinds):
        bases.append(base)
        base = base + (sum((kind_of[a] == k).astype(jnp.int32) for a in range(atoms)) + 1) // 2
    seats = []
    for a in range(atoms):
        rank = sum(((kind_of[b] == kind_of[a]).astype(jnp.int32) for b in range(a)), jnp.int32(0))
        start = sum(jnp.where(kind_of[a] == k, bases[k], 0) for k in range(kinds))
        seats.append(2 * start + rank)
        pairs[0, a] = seats[a]
    for seat in range(2 * slot_count):
        holder = sum(jnp.where(seats[a] == seat, a + 1, 0) for a in range(atoms))
        pairs[1, seat] = holder
    zero_row = jnp.zeros((1, funcs), f32)
    half = 16 if share % 16 == 0 else share

    def copies_from(source, g, s, piece):
        found = []
        for h in range(share // half) if piece is None else (piece,):
            rs = pl.ds(pl.multiple_of(g * share + h * half, 8), half)
            for side, start, target in ((0, planes - 2, right), (1, 0, left)):
                found.append(
                    pltpu.make_async_remote_copy(
                        src_ref=source.at[pl.ds(start, 2), rs],
                        dst_ref=halo.at[g, s, side, h],
                        send_sem=send_sem.at[g, side, h],
                        recv_sem=recv_sem.at[g, s, side, h],
                        device_id={"slab": target},
                        device_id_type=MESH,
                    )
                )
        return found

    for g in range(groups):
        for copy in copies_from(even, g, 0, None):
            copy.start()

    centre = scal_ref[2 * ORDER]
    quad = 4
    places = [plane_ref[a] - me * planes for a in range(atoms)]
    order = sorted(range(1, bands), key=lambda d: abs(d - bands / 2))
    unit = min(width, points)
    units = width // unit

    def outgoing(g, d, u):
        rs = pl.ds(pl.multiple_of(g * share, share), share)
        target = lax.rem(my_band + d, bands)
        if width >= points:
            src = even.at[target * units + u, rs]
        else:
            per = points // width
            src = even.at[target // per, rs, pl.ds(pl.multiple_of(lax.rem(target, per) * width, 128), width)]
        return pltpu.make_async_remote_copy(
            src_ref=src,
            dst_ref=out_ref.at[my_band, rs, u * unit : (u + 1) * unit],
            send_sem=out_sem.at[g, d - 1, u],
            recv_sem=in_sem.at[g, d - 1, u],
            device_id={"band": target},
            device_id_type=MESH,
        )

    def own(u):
        if width >= points:
            src = even.at[my_band * units + u]
        else:
            per = points // width
            src = even.at[my_band // per, :, pl.ds(pl.multiple_of(lax.rem(my_band, per) * width, 128), width)]
        return pltpu.make_async_copy(src, out_ref.at[my_band, :, u * unit : (u + 1) * unit], own_sem.at[u])

    def group_step(g, first):
        rs = pl.ds(first, share)

        def split_plane(x, c):
            high, low = halves(even[x, rs])
            split[x, :share] = high
            split[x, share:] = low
            return c

        lax.fori_loop(0, planes, split_plane, 0)

        def step(s, cur, nxt):
            scale = scal_ref[2 * s]
            pull = scal_ref[2 * s + 1]
            def pair(q, c):
                holders = [pairs[1, 2 * q + m] for m in range(2)]
                atom = [jnp.maximum(holder - 1, 0) for holder in holders]
                k = jnp.clip(kind_ref[atom[0]], 0, kinds - 1)
                places = [jnp.clip(plane_ref[atom[m]] - me * planes, 0, planes - depth) for m in range(2)]
                both = jnp.concatenate(
                    [jnp.concatenate([split[p + j] for j in range(depth)], axis=1) for p in places], axis=0
                )
                r = jnp.dot(both, table[k], preferred_element_type=f32)
                stack = []
                for m in range(2):
                    at = m * 2 * share
                    coupled = r[at : at + share, :funcs] + (
                        r[at : at + share, funcs:] + r[at + share : at + 2 * share, :funcs]
                    )
                    coef = jnp.where(holders[m] > 0, coef_ref[pl.ds(atom[m], 1)], zero_row)
                    for value in halves(coupled * coef):
                        stack.append(jnp.concatenate([value, value], axis=1))
                stack = jnp.concatenate(stack, axis=0)
                for j in range(depth):
                    r = jnp.dot(stack, back[k, :, j * points : (j + 1) * points], preferred_element_type=f32)
                    for m in range(2):
                        at = m * 2 * share
                        spread[2 * q + m, j + 1] = r[at : at + share] + r[at + share : at + 2 * share]
                return c

            lax.fori_loop(0, slot_count, pair, 0, unroll=True)

            seat_of = [pairs[0, a] for a in range(atoms)]
            slots = {x: [jnp.clip(x - places[a], -1, depth) + 1 for a in range(atoms)] for x in range(planes)}

            def quads(xs, take, before=None, after=None):
                both = jnp.concatenate([split[x] for x in xs], axis=0)
                r = jnp.dot(both, lap[...], preferred_element_type=f32)
                piece = min(16, share)
                span = min(256, points)
                for r0, l0 in [(r0, l0) for r0 in range(0, share, piece) for l0 in range(0, points, span)]:
                    ls = slice(l0, l0 + span)
                    if before is not None and r0 % half == 0 and l0 == 0:
                        before(r0 // half)
                    fs = {}
                    for x in xs:
                        for d in (-2, -1, 0, 1, 2):
                            if x + d not in fs:
                                fs[x + d] = take(x + d, r0, piece, ls)
                    for i, x in enumerate(xs):
                        base = i * 2 * share + r0
                        total = (r[base : base + piece, ls] + r[base + share : base + share + piece, ls]) * (-0.5 / 12.0)
                        total = total + (pot_ref[pl.ds(x, 1), ls] + (1.25 - centre)) * fs[x]
                        total = total + (fs[x - 1] + fs[x + 1]) * (-2.0 / 3.0) + (fs[x - 2] + fs[x + 2]) * (1.0 / 24.0)
                        for a in range(atoms):
                            total = total + spread[seat_of[a], slots[x][a], r0 : r0 + piece, ls]
                        at = (x, pl.ds(first + r0, piece), ls)
                        fresh = scale * total - pull * nxt[at]
                        nxt[at] = fresh
                        high, low = halves(fresh)
                        split[x, r0 : r0 + piece, ls] = high
                        split[x, share + r0 : share + r0 + piece, ls] = low
                    if after is not None and (r0 + piece) % half == 0 and l0 + span == points:
                        after(r0 // half)

            def take(x, r0, piece, ls):
                if x < 0:
                    return halo[g, s, 0, r0 // half, x + 2, r0 % half : r0 % half + piece, ls]
                if x >= planes:
                    return halo[g, s, 1, r0 // half, x - planes, r0 % half : r0 % half + piece, ls]
                return cur[x, pl.ds(first + r0, piece), ls]

            for x0 in range(2, planes - 2, quad):
                quads(list(range(x0, min(x0 + quad, planes - 2))), take)

            def before(h):
                for copy in copies_from(cur, g, s, h):
                    copy.wait()

            def after(h):
                @pl.when(s + 1 < ORDER)
                def _():
                    for copy in copies_from(nxt, g, s + 1, h):
                        copy.start()

            quads([0, 1, planes - 2, planes - 1], take, before, after)

        def two(i, c):
            step(2 * i, even, odd)
            step(2 * i + 1, odd, even)
            return c

        lax.fori_loop(0, ORDER // 2, two, 0)

    def run_group(g, c):
        group_step(g, pl.multiple_of(g * share, share))
        for d in order:
            for u in range(units):
                outgoing(g, d, u).start()
        return c

    lax.fori_loop(0, groups, run_group, 0)
    for u in range(units):
        own(u).start()
    for g in range(groups):
        for d in order:
            for u in range(units):
                outgoing(g, d, u).wait()
    for u in range(units):
        own(u).wait()


def filter_call(plane, kind, scal, orb, pot, coef, proj, groups):
    rows, planes, points = orb.shape
    atoms = coef.shape[0]
    kinds, block, funcs = proj.shape
    depth = block // points
    bands = lax.axis_size("band")
    share = rows // groups
    width = planes * points // bands
    units = max(width // points, 1)
    half = 16 if share % 16 == 0 else share
    smem = pl.BlockSpec(memory_space=pltpu.SMEM)
    vmem = pl.BlockSpec(memory_space=pltpu.VMEM)
    hbm = pl.BlockSpec(memory_space=pl.ANY)
    dma = pltpu.SemaphoreType.DMA
    return pl.pallas_call(
        functools.partial(filter_kernel, groups),
        out_shape=jax.ShapeDtypeStruct((bands, rows, planes * points // bands), f32),
        in_specs=[smem] * 3 + [hbm, vmem, vmem, hbm],
        out_specs=vmem,
        scratch_shapes=[
            pltpu.VMEM((kinds, block, 2 * funcs), bf16),
            pltpu.VMEM((kinds, 2 * funcs, block), bf16),
            pltpu.VMEM((points, points), bf16),
            pltpu.VMEM((planes, rows, points), f32),
            pltpu.VMEM((planes, rows, points), f32),
            pltpu.VMEM((planes, 2 * share, points), bf16),
            pltpu.VMEM((2 * pair_slots(atoms, kinds), depth + 2, share, points), f32),
            pltpu.VMEM((groups, ORDER, 2, share // half, 2, half, points), f32),
            pltpu.VMEM((kinds, block, funcs), f32),
            pltpu.SMEM((2, max(atoms, 2 * pair_slots(atoms, kinds))), jnp.int32),
            dma((planes,)),
            dma((kinds,)),
            dma((units,)),
            dma((groups, 2, share // half)),
            dma((groups, ORDER, 2, share // half)),
            dma((groups, bands - 1, units)),
            dma((groups, bands - 1, units)),
        ],
        compiler_params=pltpu.CompilerParams(
            collective_id=0, has_side_effects=True, vmem_limit_bytes=60 * 1024 * 1024
        ),
        name="cheb_filter",
    )(plane, kind, scal, orb, pot, coef, proj)


def invert_block(t_ref, cols_ref, nb):
    lanes = lax.broadcasted_iota(jnp.int32, (micro, nb), 1)
    subs = lax.broadcasted_iota(jnp.int32, (micro, nb), 0)
    for k in range(0, nb, micro):
        inside = (lanes >= k) & (lanes < k + micro)
        head = t_ref[k : k + micro, :]
        for t in range(micro):
            cols_ref[t] = jnp.broadcast_to(head[:, k + t : k + t + 1], (micro, nb))
        rows = [
            jnp.where(inside, (lanes == k + t).astype(f32), jnp.broadcast_to(t_ref[k + t : k + t + 1, :], (micro, nb)))
            for t in range(micro)
        ]
        e = {
            (s, t): jnp.broadcast_to(cols_ref[t, s : s + 1, :], (micro, nb))
            for t in range(micro)
            for s in range(t, micro)
        }
        link, inv = {}, []
        for t in range(micro):
            inv.append(1.0 / e[t, t])
            for s in range(t + 1, micro):
                link[s, t] = e[s, t] * inv[t]
            for s in range(t + 1, micro):
                for u in range(t + 1, s + 1):
                    e[s, u] = e[s, u] - link[s, t] * e[u, t]
                rows[s] = rows[s] - link[s, t] * rows[t]
        solved = [rows[t] * inv[t] for t in range(micro)]
        for s in range(micro - 1, 0, -1):
            for t in range(s):
                solved[t] = solved[t] - link[s, t] * solved[s]
        for i in range(k + micro, nb, micro):
            tile = t_ref[i : i + micro, :]
            parts = [jnp.broadcast_to(tile[:, k + t : k + t + 1], (micro, nb)) * solved[t] for t in range(micro)]
            while len(parts) > 1:
                parts = [parts[j] + parts[j + 1] for j in range(0, len(parts), 2)]
            t_ref[i : i + micro, :] = jnp.where(inside, 0.0, tile) - parts[0]
        final = jnp.zeros((micro, nb), f32)
        for t in range(micro):
            final = jnp.where(subs == t, rows[t] * lax.rsqrt(e[t, t]), final)
        t_ref[k : k + micro, :] = jnp.where(lanes < k + micro, final, 0.0)


def factor_body(nb, a_ref, w_ref, t_ref, cols_ref):
    n = w_ref.shape[0]
    nt = (((1,), (1,)), ((), ()))
    count = n // nb

    def one(b, c):
        at = pl.ds(pl.multiple_of(b * nb, nb), nb)
        t_ref[...] = a_ref[at, at]
        invert_block(t_ref, cols_ref, nb)
        for i in range(count):

            @pl.when(b == i)
            def _():
                lo, hi = i * nb, (i + 1) * nb
                inverse = t_ref[...]
                w_ref[lo:hi, lo:hi] = inverse
                if hi < n:
                    w_ref[lo:hi, hi:] = jnp.zeros((nb, n - hi), f32)
                    panel = lax.dot_general(a_ref[hi:, lo:hi], inverse, nt, precision=highest, preferred_element_type=f32)
                    a_ref[hi:, lo:hi] = panel
                    a_ref[hi:, hi:] = a_ref[hi:, hi:] - lax.dot_general(
                        panel, panel, nt, precision=highest, preferred_element_type=f32
                    )
                if lo > 0:
                    mixed = jnp.dot(a_ref[lo:hi, :lo], w_ref[:lo, :lo], precision=highest, preferred_element_type=f32)
                    w_ref[lo:hi, :lo] = -jnp.dot(inverse, mixed, precision=highest, preferred_element_type=f32)

        return c

    lax.fori_loop(0, count, one, 0)


def orthogonal_kernel(
    nb, point_total, f_ref, w_ref, stack, pack, first, part, second, full, a_ref, t_ref, cols_ref,
    pair_sems, sum_send, sum_recv, gather_send, gather_recv, relay_send, relay_recv,
):
    n = w_ref.shape[0]
    count = n // nb
    total = pack.shape[0]
    slabs, bands = lax.axis_size("slab"), lax.axis_size("band")
    my_slab, my_band = lax.axis_index("slab"), lax.axis_index("band")
    lines = slabs // 2
    chips = bands * lines
    core, chip = lax.rem(my_slab, 2), my_band * lines + my_slab // 2
    partner = my_slab + 1 - 2 * core
    deep = total // 2
    thin = deep // chips
    base = core * deep

    barrier = pltpu.get_barrier_semaphore()

    def place(d):
        other = lax.rem(chip + d, chips)
        return other, {"band": other // lines, "slab": lax.rem(other, lines) * 2 + core}

    def greet(d, c):
        pl.semaphore_signal(barrier, inc=1, device_id=place(d)[1], device_id_type=MESH)
        return c

    pl.semaphore_signal(barrier, inc=1, device_id={"slab": partner}, device_id_type=MESH)
    lax.fori_loop(1, chips, greet, 0)

    for i in range(count):
        rows = pl.ds(i * nb, nb)
        high, low = halves(f_ref[rows, :])
        stack[i, :nb] = high
        stack[i, nb:] = low
    at = 0
    for j in range(count):
        for i in range(j, count):
            r = lax.dot_general(stack[i], stack[j], (((1,), (1,)), ((), ())), preferred_element_type=f32)
            r = (r[:nb, :nb] + r[nb:, nb:]) + (r[:nb, nb:] + r[nb:, :nb])
            pack[at : at + nb] = r * (1.0 / point_total)
            at += nb
    if at < total:
        pack[at:] = jnp.zeros((total - at, nb), f32)

    pl.semaphore_wait(barrier, chips)

    def span(start, length):
        return pl.ds(pl.multiple_of(start, 8), length)

    swap = pltpu.make_async_remote_copy(
        src_ref=pack.at[span((1 - core) * deep, deep)], dst_ref=first, send_sem=pair_sems.at[0],
        recv_sem=pair_sems.at[1], device_id={"slab": partner}, device_id_type=MESH,
    )
    swap.start()
    swap.wait()
    part[...] = pack[span(base, deep)] + first[...]

    def scatter(d):
        other, device = place(d)
        return pltpu.make_async_remote_copy(
            src_ref=part.at[span(other * thin, thin)], dst_ref=second.at[d - 1], send_sem=sum_send.at[d - 1],
            recv_sem=sum_recv.at[d - 1], device_id=device, device_id_type=MESH,
        )

    def mine(c):
        return span(base + c * thin, thin)

    def gather(d):
        return pltpu.make_async_remote_copy(
            src_ref=full.at[mine(chip)], dst_ref=full.at[mine(chip)], send_sem=gather_send.at[d - 1],
            recv_sem=gather_recv.at[d - 1], device_id=place(d)[1], device_id_type=MESH,
        )

    def relay(d):
        rows = mine(lax.rem(chip + chips - d, chips))
        return pltpu.make_async_remote_copy(
            src_ref=full.at[rows], dst_ref=full.at[rows], send_sem=relay_send.at[d], recv_sem=relay_recv.at[d],
            device_id={"slab": partner}, device_id_type=MESH,
        )

    def each(first_index, action):
        def body(d, c):
            action(d)
            return c

        lax.fori_loop(first_index, chips, body, 0)

    each(1, lambda d: scatter(d).start())
    each(1, lambda d: scatter(d).wait())

    def accumulate(d, value):
        return value + second[d - 1]

    full[mine(chip)] = lax.fori_loop(1, chips, accumulate, part[span(chip * thin, thin)])
    each(1, lambda d: gather(d).start())
    relay(0).start()

    def pass_on(d):
        gather(d).wait()
        relay(d).start()

    each(1, pass_on)
    each(0, lambda d: relay(d).wait())

    a_ref[...] = jnp.zeros((n, n), f32)
    at = 0
    for j in range(count):
        for i in range(j, count):
            a_ref[i * nb : (i + 1) * nb, j * nb : (j + 1) * nb] = full[at : at + nb]
            at += nb
    factor_body(nb, a_ref, w_ref, t_ref, cols_ref)


def inverse_factor(grid_layout):
    n, width = grid_layout.shape
    nb = 128 if n % 128 == 0 else n
    slabs, bands = lax.axis_size("slab"), lax.axis_size("band")
    chips = bands * slabs // 2
    count = n // nb
    used = count * (count + 1) // 2 * nb
    unit = 16 * chips
    total = (used + unit - 1) // unit * unit
    vmem = pl.BlockSpec(memory_space=pltpu.VMEM)
    dma = pltpu.SemaphoreType.DMA
    return pl.pallas_call(
        functools.partial(orthogonal_kernel, nb, width * slabs * bands),
        out_shape=jax.ShapeDtypeStruct((n, n), f32),
        in_specs=[vmem],
        out_specs=vmem,
        scratch_shapes=[
            pltpu.VMEM((count, 2 * nb, width), bf16),
            pltpu.VMEM((total, nb), f32),
            pltpu.VMEM((total // 2, nb), f32),
            pltpu.VMEM((total // 2, nb), f32),
            pltpu.VMEM((chips - 1, total // 2 // chips, nb), f32),
            pltpu.VMEM((total, nb), f32),
            pltpu.VMEM((n, n), f32),
            pltpu.VMEM((nb, nb), f32),
            pltpu.VMEM((micro, micro, nb), f32),
            dma((2,)),
            dma((chips - 1,)),
            dma((chips - 1,)),
            dma((chips - 1,)),
            dma((chips - 1,)),
            dma((chips,)),
            dma((chips,)),
        ],
        compiler_params=pltpu.CompilerParams(
            collective_id=1, has_side_effects=True, vmem_limit_bytes=32 * 1024 * 1024
        ),
        name="gram_factor",
    )(grid_layout)


def local(
    orbitals, potential, projectors, atom_kind, atom_plane, atom_coef, filter_cut, filter_top
):
    rows = orbitals.shape[0]
    centre, pairs = chebyshev_scalars(filter_cut[0], filter_top[0])
    scal = []
    for a, b in pairs:
        scal += [a, jnp.zeros((), f32) if b is None else b]
    scal = jnp.stack(scal + [centre])
    filtered = filter_call(
        atom_plane, atom_kind, scal, orbitals, potential, atom_coef, projectors, 2 if rows % 32 == 0 else 1
    )
    grid_layout = filtered.reshape(-1, filtered.shape[2])
    factor_inverse = inverse_factor(grid_layout)
    return jnp.dot(factor_inverse, grid_layout, precision=lax.Precision.HIGH)


def solution(mesh):
    in_specs = (
        P("band", "slab", None),
        P("slab", None),
        P(),
        P("slab"),
        P("slab"),
        P("slab", None),
        P(),
        P(),
    )
    out_specs = P(None, ("slab", "band"))
    return jax.shard_map(local, mesh=mesh, in_specs=in_specs, out_specs=out_specs, check_vma=False)
```

```python
import functools
import jax
import jax.numpy as jnp
from jax import lax
from jax.experimental import pallas as pl
from jax.experimental.pallas import tpu as pltpu
from jax.sharding import PartitionSpec as P

GZ = 32
ORDER = 6
micro = 8

low_edge = -1.0
highest = lax.Precision.HIGHEST
f32 = jnp.float32
bf16 = jnp.bfloat16
MESH = pl.DeviceIdType.MESH


def halves(value):
    high = value.astype(bf16)
    return high, (value - high.astype(f32)).astype(bf16)


def chebyshev_scalars(cut, top):
    half = (top - cut) / 2.0
    centre = (top + cut) / 2.0
    sigma = half / (low_edge - centre)
    tau = 2.0 / sigma
    pairs = [(sigma / half, None)]
    for _ in range(ORDER - 1):
        following = 1.0 / (tau - sigma)
        pairs.append((2.0 * following / half, sigma * following))
        sigma = following
    return centre, pairs


def pair_slots(atoms, kinds):
    return min(atoms, (atoms + kinds) // 2)


def filter_kernel(
    groups, plane_ref, kind_ref, scal_ref, orb_ref, pot_ref, coef_ref, proj_ref,
    out_ref, table, back, lap, even, odd, split, spread, halo, raw, pairs, load_sem, table_sem, own_sem,
    send_sem, recv_sem, out_sem, in_sem,
):
    rows, planes, points = orb_ref.shape
    kinds, block, funcs = proj_ref.shape
    atoms = coef_ref.shape[0]
    depth = block // points
    share = rows // groups
    width = out_ref.shape[2]
    slabs, bands = lax.axis_size("slab"), lax.axis_size("band")
    me, my_band = lax.axis_index("slab"), lax.axis_index("band")
    right, left = lax.rem(me + 1, slabs), lax.rem(me + slabs - 1, slabs)

    loads = []
    for x in range(planes):
        loads.append(pltpu.make_async_copy(orb_ref.at[:, x], even.at[x], load_sem.at[x]))
        loads[-1].start()
    tables = []
    for k in range(kinds):
        tables.append(pltpu.make_async_copy(proj_ref.at[k], raw.at[k], table_sem.at[k]))
        tables[-1].start()

    barrier = pltpu.get_barrier_semaphore()
    for neighbour in (left, right):
        pl.semaphore_signal(barrier, inc=1, device_id={"slab": neighbour}, device_id_type=MESH)
    for d in range(1, bands):
        pl.semaphore_signal(barrier, inc=1, device_id={"band": lax.rem(my_band + d, bands)}, device_id_type=MESH)

    zeros = jnp.zeros((rows, points), f32)

    def clear(x, c):
        odd[x] = zeros
        return c

    lax.fori_loop(0, planes, clear, 0)

    def clear_spread(a, c):
        spread[a, 0] = zeros[:share]
        spread[a, depth + 1] = zeros[:share]
        return c

    lax.fori_loop(0, spread.shape[0], clear_spread, 0)

    strip = 64

    def lap_rows(i, c):
        r = lax.broadcasted_iota(jnp.int32, (strip, points), 0) + i * strip
        q = lax.broadcasted_iota(jnp.int32, (strip, points), 1)
        dy = jnp.abs(r // GZ - q // GZ)
        dz = jnp.abs(r % GZ - q % GZ)

        def line(d):
            return jnp.where(d == 0, -30.0, jnp.where(d == 1, 16.0, jnp.where(d == 2, -1.0, 0.0)))

        lap[pl.ds(i * strip, strip)] = (jnp.where(dz == 0, line(dy), 0.0) + jnp.where(dy == 0, line(dz), 0.0)).astype(bf16)
        return c

    lax.fori_loop(0, points // strip, lap_rows, 0)

    part = 256

    for k in range(kinds):
        tables[k].wait()

        def convert(i, c):
            at = pl.ds(i * part, part)
            high, low = halves(raw[k, at])
            table[k, at, :funcs] = high
            table[k, at, funcs:] = low
            lanes = pl.ds(pl.multiple_of(i * part, part), part)
            back[k, :funcs, lanes] = high.T
            back[k, funcs:, lanes] = low.T
            return c

        lax.fori_loop(0, block // part, convert, 0)

    for copy in loads:
        copy.wait()

    slot_count = pair_slots(atoms, kinds)
    kind_of = [jnp.clip(kind_ref[a], 0, kinds - 1) for a in range(atoms)]
    base, bases = 0, []
    for k in range(kinds):
        bases.append(base)
        base = base + (sum((kind_of[a] == k).astype(jnp.int32) for a in range(atoms)) + 1) // 2
    seats = []
    for a in range(atoms):
        rank = sum(((kind_of[b] == kind_of[a]).astype(jnp.int32) for b in range(a)), jnp.int32(0))
        start = sum(jnp.where(kind_of[a] == k, bases[k], 0) for k in range(kinds))
        seats.append(2 * start + rank)
        pairs[0, a] = seats[a]
    for seat in range(2 * slot_count):
        holder = sum(jnp.where(seats[a] == seat, a + 1, 0) for a in range(atoms))
        pairs[1, seat] = holder
    zero_row = jnp.zeros((1, funcs), f32)
    half = 16 if share % 16 == 0 else share

    def copies_from(source, g, s, piece):
        found = []
        for h in range(share // half) if piece is None else (piece,):
            rs = pl.ds(pl.multiple_of(g * share + h * half, 8), half)
            for side, start, target in ((0, planes - 2, right), (1, 0, left)):
                found.append(
                    pltpu.make_async_remote_copy(
                        src_ref=source.at[pl.ds(start, 2), rs],
                        dst_ref=halo.at[g, s, side, h],
                        send_sem=send_sem.at[g, side, h],
                        recv_sem=recv_sem.at[g, s, side, h],
                        device_id={"slab": target},
                        device_id_type=MESH,
                    )
                )
        return found

    pl.semaphore_wait(barrier, bands + 1)
    for g in range(groups):
        for copy in copies_from(even, g, 0, None):
            copy.start()

    centre = scal_ref[2 * ORDER]
    quad = 4
    places = [plane_ref[a] - me * planes for a in range(atoms)]
    order = sorted(range(1, bands), key=lambda d: abs(d - bands / 2))
    unit = min(width, points)
    units = width // unit

    def outgoing(g, d, u):
        rs = pl.ds(pl.multiple_of(g * share, share), share)
        target = lax.rem(my_band + d, bands)
        if width >= points:
            src = even.at[target * units + u, rs]
        else:
            per = points // width
            src = even.at[target // per, rs, pl.ds(pl.multiple_of(lax.rem(target, per) * width, 128), width)]
        return pltpu.make_async_remote_copy(
            src_ref=src,
            dst_ref=out_ref.at[my_band, rs, u * unit : (u + 1) * unit],
            send_sem=out_sem.at[g, d - 1, u],
            recv_sem=in_sem.at[g, d - 1, u],
            device_id={"band": target},
            device_id_type=MESH,
        )

    def own(u):
        if width >= points:
            src = even.at[my_band * units + u]
        else:
            per = points // width
            src = even.at[my_band // per, :, pl.ds(pl.multiple_of(lax.rem(my_band, per) * width, 128), width)]
        return pltpu.make_async_copy(src, out_ref.at[my_band, :, u * unit : (u + 1) * unit], own_sem.at[u])

    def group_step(g, first):
        rs = pl.ds(first, share)

        def split_plane(x, c):
            high, low = halves(even[x, rs])
            split[x, :share] = high
            split[x, share:] = low
            return c

        lax.fori_loop(0, planes, split_plane, 0)

        def step(s, cur, nxt):
            scale = scal_ref[2 * s]
            pull = scal_ref[2 * s + 1]
            def pair(q, c):
                holders = [pairs[1, 2 * q + m] for m in range(2)]
                atom = [jnp.maximum(holder - 1, 0) for holder in holders]
                k = jnp.clip(kind_ref[atom[0]], 0, kinds - 1)
                places = [jnp.clip(plane_ref[atom[m]] - me * planes, 0, planes - depth) for m in range(2)]
                both = jnp.concatenate(
                    [jnp.concatenate([split[p + j] for j in range(depth)], axis=1) for p in places], axis=0
                )
                r = jnp.dot(both, table[k], preferred_element_type=f32)
                stack = []
                for m in range(2):
                    at = m * 2 * share
                    coupled = r[at : at + share, :funcs] + (
                        r[at : at + share, funcs:] + r[at + share : at + 2 * share, :funcs]
                    )
                    coef = jnp.where(holders[m] > 0, coef_ref[pl.ds(atom[m], 1)], zero_row)
                    for value in halves(coupled * coef):
                        stack.append(jnp.concatenate([value, value], axis=1))
                stack = jnp.concatenate(stack, axis=0)
                for j in range(depth):
                    r = jnp.dot(stack, back[k, :, j * points : (j + 1) * points], preferred_element_type=f32)
                    for m in range(2):
                        at = m * 2 * share
                        spread[2 * q + m, j + 1] = r[at : at + share] + r[at + share : at + 2 * share]
                return c

            lax.fori_loop(0, slot_count, pair, 0, unroll=True)

            seat_of = [pairs[0, a] for a in range(atoms)]
            slots = {x: [jnp.clip(x - places[a], -1, depth) + 1 for a in range(atoms)] for x in range(planes)}

            def quads(xs, take, first_row, count):
                both = jnp.concatenate(
                    [split[x, base + first_row : base + first_row + count] for x in xs for base in (0, share)], axis=0
                )
                r = jnp.dot(both, lap[...], preferred_element_type=f32)
                piece = min(16, share)
                span = min(256, points)
                for r0, l0 in [(r0, l0) for r0 in range(first_row, first_row + count, piece) for l0 in range(0, points, span)]:
                    ls = slice(l0, l0 + span)
                    fs = {}
                    for x in xs:
                        for d in (-2, -1, 0, 1, 2):
                            if x + d not in fs:
                                fs[x + d] = take(x + d, r0, piece, ls)
                    for i, x in enumerate(xs):
                        base = i * 2 * count + r0 - first_row
                        total = (r[base : base + piece, ls] + r[base + count : base + count + piece, ls]) * (-0.5 / 12.0)
                        total = total + (pot_ref[pl.ds(x, 1), ls] + (1.25 - centre)) * fs[x]
                        total = total + (fs[x - 1] + fs[x + 1]) * (-2.0 / 3.0) + (fs[x - 2] + fs[x + 2]) * (1.0 / 24.0)
                        for a in range(atoms):
                            total = total + spread[seat_of[a], slots[x][a], r0 : r0 + piece, ls]
                        at = (x, pl.ds(first + r0, piece), ls)
                        fresh = scale * total - pull * nxt[at]
                        nxt[at] = fresh
                        high, low = halves(fresh)
                        split[x, r0 : r0 + piece, ls] = high
                        split[x, share + r0 : share + r0 + piece, ls] = low

            def take(x, r0, piece, ls):
                if x < 0:
                    return halo[g, s, 0, r0 // half, x + 2, r0 % half : r0 % half + piece, ls]
                if x >= planes:
                    return halo[g, s, 1, r0 // half, x - planes, r0 % half : r0 % half + piece, ls]
                return cur[x, pl.ds(first + r0, piece), ls]

            def before(h):
                for copy in copies_from(cur, g, s, h):
                    copy.wait()

            def after(h):
                @pl.when(s + 1 < ORDER)
                def _():
                    for copy in copies_from(nxt, g, s + 1, h):
                        copy.start()

            for h in range(share // half):
                before(h)
                quads([0, 1, planes - 2, planes - 1], take, h * half, half)
                after(h)
                if h == 0:
                    for x0 in range(2, planes - 2, quad):
                        quads(list(range(x0, min(x0 + quad, planes - 2))), take, 0, share)

        def two(i, c):
            step(2 * i, even, odd)
            step(2 * i + 1, odd, even)
            return c

        lax.fori_loop(0, ORDER // 2, two, 0)

    def run_group(g, c):
        group_step(g, pl.multiple_of(g * share, share))
        for d in order:
            for u in range(units):
                outgoing(g, d, u).start()
        return c

    lax.fori_loop(0, groups, run_group, 0)
    for u in range(units):
        own(u).start()
    for g in range(groups):
        for d in order:
            for u in range(units):
                outgoing(g, d, u).wait()
    for u in range(units):
        own(u).wait()


def filter_call(plane, kind, scal, orb, pot, coef, proj, groups):
    rows, planes, points = orb.shape
    atoms = coef.shape[0]
    kinds, block, funcs = proj.shape
    depth = block // points
    bands = lax.axis_size("band")
    share = rows // groups
    width = planes * points // bands
    units = max(width // points, 1)
    half = 16 if share % 16 == 0 else share
    smem = pl.BlockSpec(memory_space=pltpu.SMEM)
    vmem = pl.BlockSpec(memory_space=pltpu.VMEM)
    hbm = pl.BlockSpec(memory_space=pl.ANY)
    dma = pltpu.SemaphoreType.DMA
    return pl.pallas_call(
        functools.partial(filter_kernel, groups),
        out_shape=jax.ShapeDtypeStruct((bands, rows, planes * points // bands), f32),
        in_specs=[smem] * 3 + [hbm, vmem, vmem, hbm],
        out_specs=vmem,
        scratch_shapes=[
            pltpu.VMEM((kinds, block, 2 * funcs), bf16),
            pltpu.VMEM((kinds, 2 * funcs, block), bf16),
            pltpu.VMEM((points, points), bf16),
            pltpu.VMEM((planes, rows, points), f32),
            pltpu.VMEM((planes, rows, points), f32),
            pltpu.VMEM((planes, 2 * share, points), bf16),
            pltpu.VMEM((2 * pair_slots(atoms, kinds), depth + 2, share, points), f32),
            pltpu.VMEM((groups, ORDER, 2, share // half, 2, half, points), f32),
            pltpu.VMEM((kinds, block, funcs), f32),
            pltpu.SMEM((2, max(atoms, 2 * pair_slots(atoms, kinds))), jnp.int32),
            dma((planes,)),
            dma((kinds,)),
            dma((units,)),
            dma((groups, 2, share // half)),
            dma((groups, ORDER, 2, share // half)),
            dma((groups, bands - 1, units)),
            dma((groups, bands - 1, units)),
        ],
        compiler_params=pltpu.CompilerParams(
            collective_id=0, has_side_effects=True, vmem_limit_bytes=60 * 1024 * 1024
        ),
        name="cheb_filter",
    )(plane, kind, scal, orb, pot, coef, proj)


def invert_block(t_ref, cols_ref, nb):
    lanes = lax.broadcasted_iota(jnp.int32, (micro, nb), 1)
    subs = lax.broadcasted_iota(jnp.int32, (micro, nb), 0)
    for k in range(0, nb, micro):
        inside = (lanes >= k) & (lanes < k + micro)
        head = t_ref[k : k + micro, :]
        for t in range(micro):
            cols_ref[t] = jnp.broadcast_to(head[:, k + t : k + t + 1], (micro, nb))
        rows = [
            jnp.where(inside, (lanes == k + t).astype(f32), jnp.broadcast_to(t_ref[k + t : k + t + 1, :], (micro, nb)))
            for t in range(micro)
        ]
        e = {
            (s, t): jnp.broadcast_to(cols_ref[t, s : s + 1, :], (micro, nb))
            for t in range(micro)
            for s in range(t, micro)
        }
        link, inv = {}, []
        for t in range(micro):
            inv.append(1.0 / e[t, t])
            for s in range(t + 1, micro):
                link[s, t] = e[s, t] * inv[t]
            for s in range(t + 1, micro):
                for u in range(t + 1, s + 1):
                    e[s, u] = e[s, u] - link[s, t] * e[u, t]
                rows[s] = rows[s] - link[s, t] * rows[t]
        solved = [rows[t] * inv[t] for t in range(micro)]
        for s in range(micro - 1, 0, -1):
            for t in range(s):
                solved[t] = solved[t] - link[s, t] * solved[s]
        for i in range(k + micro, nb, micro):
            tile = t_ref[i : i + micro, :]
            parts = [jnp.broadcast_to(tile[:, k + t : k + t + 1], (micro, nb)) * solved[t] for t in range(micro)]
            while len(parts) > 1:
                parts = [parts[j] + parts[j + 1] for j in range(0, len(parts), 2)]
            t_ref[i : i + micro, :] = jnp.where(inside, 0.0, tile) - parts[0]
        final = jnp.zeros((micro, nb), f32)
        for t in range(micro):
            final = jnp.where(subs == t, rows[t] * lax.rsqrt(e[t, t]), final)
        t_ref[k : k + micro, :] = jnp.where(lanes < k + micro, final, 0.0)


def factor_body(nb, a_ref, w_ref, t_ref, cols_ref, complete):
    n = w_ref.shape[0]
    nt = (((1,), (1,)), ((), ()))
    count = n // nb

    def one(b, c):
        at = pl.ds(pl.multiple_of(b * nb, nb), nb)
        t_ref[...] = a_ref[at, at]
        invert_block(t_ref, cols_ref, nb)
        pl.when(b == 0)(complete)
        for i in range(count):

            @pl.when(b == i)
            def _():
                lo, hi = i * nb, (i + 1) * nb
                inverse = t_ref[...]
                w_ref[lo:hi, lo:hi] = inverse
                if hi < n:
                    w_ref[lo:hi, hi:] = jnp.zeros((nb, n - hi), f32)
                    panel = lax.dot_general(a_ref[hi:, lo:hi], inverse, nt, precision=highest, preferred_element_type=f32)
                    a_ref[hi:, lo:hi] = panel
                    a_ref[hi:, hi:] = a_ref[hi:, hi:] - lax.dot_general(
                        panel, panel, nt, precision=highest, preferred_element_type=f32
                    )
                if lo > 0:
                    mixed = jnp.dot(a_ref[lo:hi, :lo], w_ref[:lo, :lo], precision=highest, preferred_element_type=f32)
                    w_ref[lo:hi, :lo] = -jnp.dot(inverse, mixed, precision=highest, preferred_element_type=f32)

        return c

    lax.fori_loop(0, count, one, 0)


def orthogonal_kernel(
    nb, point_total, f_ref, w_ref, stack, pack, first, part, second, full, a_ref, t_ref, cols_ref,
    pair_sems, sum_send, sum_recv, gather_send, gather_recv, relay_send, relay_recv,
):
    n = w_ref.shape[0]
    count = n // nb
    slabs, bands = lax.axis_size("slab"), lax.axis_size("band")
    my_slab, my_band = lax.axis_index("slab"), lax.axis_index("band")
    lines = slabs // 2
    chips = bands * lines
    core, chip = lax.rem(my_slab, 2), my_band * lines + my_slab // 2
    partner = my_slab + 1 - 2 * core
    sections = gram_sections(count, nb, chips)

    barrier = pltpu.get_barrier_semaphore()

    def place(d):
        other = lax.rem(chip + d, chips)
        return other, {"band": other // lines, "slab": lax.rem(other, lines) * 2 + core}

    def greet(d, c):
        pl.semaphore_signal(barrier, inc=1, device_id=place(d)[1], device_id_type=MESH)
        return c

    pl.semaphore_signal(barrier, inc=1, device_id={"slab": partner}, device_id_type=MESH)
    lax.fori_loop(1, chips, greet, 0)

    for i in range(count):
        rows = pl.ds(i * nb, nb)
        high, low = halves(f_ref[rows, :])
        stack[i, :nb] = high
        stack[i, nb:] = low
    for start, size, blocks in sections:
        at = start
        for i, j in blocks:
            r = lax.dot_general(stack[i], stack[j], (((1,), (1,)), ((), ())), preferred_element_type=f32)
            r = (r[:nb, :nb] + r[nb:, nb:]) + (r[:nb, nb:] + r[nb:, :nb])
            pack[at : at + nb] = r * (1.0 / point_total)
            at += nb
        if at < start + size:
            pack[at : start + size] = jnp.zeros((start + size - at, nb), f32)
    a_ref[...] = jnp.zeros((n, n), f32)

    pl.semaphore_wait(barrier, chips)

    def span(start, length):
        return pl.ds(pl.multiple_of(start, 8), length)

    def each(first_index, action):
        def body(d, c):
            action(d)
            return c

        lax.fori_loop(first_index, chips, body, 0)

    class Section:
        def __init__(self, index):
            self.index = index
            start, size, self.blocks = sections[index]
            self.start, self.deep = start, size // 2
            self.thin = self.deep // chips
            self.low = start // 2
            self.base = start + core * self.deep
            self.row = sum(sections[i][1] for i in range(index)) // 2 // chips

        def swap(self):
            return pltpu.make_async_remote_copy(
                src_ref=pack.at[span(self.start + (1 - core) * self.deep, self.deep)],
                dst_ref=first.at[pl.ds(self.low, self.deep)],
                send_sem=pair_sems.at[self.index, 0], recv_sem=pair_sems.at[self.index, 1],
                device_id={"slab": partner}, device_id_type=MESH,
            )

        def combine(self):
            own = pl.ds(self.low, self.deep)
            part[own] = pack[span(self.base, self.deep)] + first[own]

        def scatter(self, d):
            other, device = place(d)
            return pltpu.make_async_remote_copy(
                src_ref=part.at[span(self.low + other * self.thin, self.thin)],
                dst_ref=second.at[d - 1, self.row : self.row + self.thin],
                send_sem=sum_send.at[self.index, d - 1], recv_sem=sum_recv.at[self.index, d - 1],
                device_id=device, device_id_type=MESH,
            )

        def mine(self, c):
            return span(self.base + c * self.thin, self.thin)

        def total(self):
            def accumulate(d, value):
                return value + second[d - 1, self.row : self.row + self.thin]

            full[self.mine(chip)] = lax.fori_loop(
                1, chips, accumulate, part[span(self.low + chip * self.thin, self.thin)]
            )

        def gather(self, d):
            return pltpu.make_async_remote_copy(
                src_ref=full.at[self.mine(chip)], dst_ref=full.at[self.mine(chip)],
                send_sem=gather_send.at[self.index, d - 1], recv_sem=gather_recv.at[self.index, d - 1],
                device_id=place(d)[1], device_id_type=MESH,
            )

        def relay(self, d):
            rows = self.mine(lax.rem(chip + chips - d, chips))
            return pltpu.make_async_remote_copy(
                src_ref=full.at[rows], dst_ref=full.at[rows], send_sem=relay_send.at[self.index, d],
                recv_sem=relay_recv.at[self.index, d], device_id={"slab": partner}, device_id_type=MESH,
            )

        def publish(self):
            self.total()
            each(1, lambda d: self.gather(d).start())
            self.relay(0).start()

        def finish(self):
            def pass_on(d):
                self.gather(d).wait()
                self.relay(d).start()

            each(1, pass_on)
            each(0, lambda d: self.relay(d).wait())
            at = self.start
            for i, j in self.blocks:
                a_ref[i * nb : (i + 1) * nb, j * nb : (j + 1) * nb] = full[at : at + nb]
                at += nb

    parts = [Section(index) for index in range(len(sections))]
    for section in parts:
        section.swap().start()
    for section in parts:
        section.swap().wait()
        section.combine()
        each(1, lambda d: section.scatter(d).start())
    for section in parts:
        each(1, lambda d: section.scatter(d).wait())
        section.publish()
    parts[0].finish()

    def complete():
        for section in parts[1:]:
            section.finish()

    factor_body(nb, a_ref, w_ref, t_ref, cols_ref, complete)


def gram_sections(count, nb, chips):
    unit = 16 * chips
    found, start = [], 0
    for blocks in (
        [(i, 0) for i in range(count)],
        [(i, j) for j in range(1, count) for i in range(j, count)],
    ):
        size = (len(blocks) * nb + unit - 1) // unit * unit
        if blocks:
            found.append((start, size, blocks))
            start += size
    return found


def inverse_factor(grid_layout):
    n, width = grid_layout.shape
    nb = 128 if n % 128 == 0 else n
    slabs, bands = lax.axis_size("slab"), lax.axis_size("band")
    chips = bands * slabs // 2
    count = n // nb
    sections = gram_sections(count, nb, chips)
    total = sum(size for _, size, _ in sections)
    parts = len(sections)
    vmem = pl.BlockSpec(memory_space=pltpu.VMEM)
    dma = pltpu.SemaphoreType.DMA
    return pl.pallas_call(
        functools.partial(orthogonal_kernel, nb, width * slabs * bands),
        out_shape=jax.ShapeDtypeStruct((n, n), f32),
        in_specs=[vmem],
        out_specs=vmem,
        scratch_shapes=[
            pltpu.VMEM((count, 2 * nb, width), bf16),
            pltpu.VMEM((total, nb), f32),
            pltpu.VMEM((total // 2, nb), f32),
            pltpu.VMEM((total // 2, nb), f32),
            pltpu.VMEM((chips - 1, total // 2 // chips, nb), f32),
            pltpu.VMEM((total, nb), f32),
            pltpu.VMEM((n, n), f32),
            pltpu.VMEM((nb, nb), f32),
            pltpu.VMEM((micro, micro, nb), f32),
            dma((parts, 2)),
            dma((parts, chips - 1)),
            dma((parts, chips - 1)),
            dma((parts, chips - 1)),
            dma((parts, chips - 1)),
            dma((parts, chips)),
            dma((parts, chips)),
        ],
        compiler_params=pltpu.CompilerParams(
            collective_id=1, has_side_effects=True, vmem_limit_bytes=32 * 1024 * 1024
        ),
        name="gram_factor",
    )(grid_layout)


def local(
    orbitals, potential, projectors, atom_kind, atom_plane, atom_coef, filter_cut, filter_top
):
    rows = orbitals.shape[0]
    centre, pairs = chebyshev_scalars(filter_cut[0], filter_top[0])
    scal = []
    for a, b in pairs:
        scal += [a, jnp.zeros((), f32) if b is None else b]
    scal = jnp.stack(scal + [centre])
    filtered = filter_call(
        atom_plane, atom_kind, scal, orbitals, potential, atom_coef, projectors, 2 if rows % 32 == 0 else 1
    )
    grid_layout = filtered.reshape(-1, filtered.shape[2])
    factor_inverse = inverse_factor(grid_layout)
    return jnp.dot(factor_inverse, grid_layout, precision=lax.Precision.HIGH)


def solution(mesh):
    in_specs = (
        P("band", "slab", None),
        P("slab", None),
        P(),
        P("slab"),
        P("slab"),
        P("slab", None),
        P(),
        P(),
    )
    out_specs = P(None, ("slab", "band"))
    return jax.shard_map(local, mesh=mesh, in_specs=in_specs, out_specs=out_specs, check_vma=False)
```

```python
import functools
import jax
import jax.numpy as jnp
from jax import lax
from jax.experimental import pallas as pl
from jax.experimental.pallas import tpu as pltpu
from jax.sharding import PartitionSpec as P

GZ = 32
ORDER = 6
micro = 8

low_edge = -1.0
highest = lax.Precision.HIGHEST
f32 = jnp.float32
bf16 = jnp.bfloat16
MESH = pl.DeviceIdType.MESH


def halves(value):
    high = value.astype(bf16)
    return high, (value - high.astype(f32)).astype(bf16)


def chebyshev_scalars(cut, top):
    half = (top - cut) / 2.0
    centre = (top + cut) / 2.0
    sigma = half / (low_edge - centre)
    tau = 2.0 / sigma
    pairs = [(sigma / half, None)]
    for _ in range(ORDER - 1):
        following = 1.0 / (tau - sigma)
        pairs.append((2.0 * following / half, sigma * following))
        sigma = following
    return centre, pairs


def pair_slots(atoms, kinds):
    return min(atoms, (atoms + kinds) // 2)


def filter_kernel(
    groups, plane_ref, kind_ref, cut_ref, top_ref, orb_ref, pot_ref, coef_ref, proj_ref,
    out_ref, table, back, lap, even, odd, split, spread, halo, raw, pairs, scal_ref, load_sem, table_sem, own_sem,
    send_sem, recv_sem, out_sem, in_sem,
):
    rows, planes, points = orb_ref.shape
    kinds, block, funcs = proj_ref.shape
    atoms = coef_ref.shape[0]
    depth = block // points
    share = rows // groups
    width = out_ref.shape[2]
    slabs, bands = lax.axis_size("slab"), lax.axis_size("band")
    me, my_band = lax.axis_index("slab"), lax.axis_index("band")
    right, left = lax.rem(me + 1, slabs), lax.rem(me + slabs - 1, slabs)

    tables = []
    for k in range(kinds):
        tables.append(pltpu.make_async_copy(proj_ref.at[k], raw.at[k], table_sem.at[k]))
        tables[-1].start()
    loads = []
    for x in range(planes):
        loads.append(pltpu.make_async_copy(orb_ref.at[:, x], even.at[x], load_sem.at[x]))
        loads[-1].start()

    barrier = pltpu.get_barrier_semaphore()
    for neighbour in (left, right):
        pl.semaphore_signal(barrier, inc=1, device_id={"slab": neighbour}, device_id_type=MESH)
    for d in range(1, bands):
        pl.semaphore_signal(barrier, inc=1, device_id={"band": lax.rem(my_band + d, bands)}, device_id_type=MESH)

    zeros = jnp.zeros((rows, points), f32)

    def clear(x, c):
        odd[x] = zeros
        return c

    lax.fori_loop(0, planes, clear, 0)

    def clear_spread(a, c):
        spread[a, 0] = zeros[:share]
        spread[a, depth + 1] = zeros[:share]
        return c

    lax.fori_loop(0, spread.shape[0], clear_spread, 0)

    strip = 64

    def lap_rows(i, c):
        r = lax.broadcasted_iota(jnp.int32, (strip, points), 0) + i * strip
        q = lax.broadcasted_iota(jnp.int32, (strip, points), 1)
        dy = jnp.abs(r // GZ - q // GZ)
        dz = jnp.abs(r % GZ - q % GZ)

        def line(d):
            return jnp.where(d == 0, -30.0, jnp.where(d == 1, 16.0, jnp.where(d == 2, -1.0, 0.0)))

        lap[pl.ds(i * strip, strip)] = (jnp.where(dz == 0, line(dy), 0.0) + jnp.where(dy == 0, line(dz), 0.0)).astype(bf16)
        return c

    lax.fori_loop(0, points // strip, lap_rows, 0)

    part = 256

    for k in range(kinds):
        tables[k].wait()

        def convert(i, c):
            at = pl.ds(i * part, part)
            high, low = halves(raw[k, at])
            table[k, at, :funcs] = high
            table[k, at, funcs:] = low
            lanes = pl.ds(pl.multiple_of(i * part, part), part)
            back[k, :funcs, lanes] = high.T
            back[k, funcs:, lanes] = low.T
            return c

        lax.fori_loop(0, block // part, convert, 0)

    for copy in loads:
        copy.wait()

    centre, steps = chebyshev_scalars(cut_ref[0], top_ref[0])
    for i, (scale, pull) in enumerate(steps):
        scal_ref[2 * i] = scale
        scal_ref[2 * i + 1] = jnp.float32(0.0) if pull is None else pull

    slot_count = pair_slots(atoms, kinds)
    kind_of = [jnp.clip(kind_ref[a], 0, kinds - 1) for a in range(atoms)]
    base, bases = 0, []
    for k in range(kinds):
        bases.append(base)
        base = base + (sum((kind_of[a] == k).astype(jnp.int32) for a in range(atoms)) + 1) // 2
    seats = []
    for a in range(atoms):
        rank = sum(((kind_of[b] == kind_of[a]).astype(jnp.int32) for b in range(a)), jnp.int32(0))
        start = sum(jnp.where(kind_of[a] == k, bases[k], 0) for k in range(kinds))
        seats.append(2 * start + rank)
        pairs[0, a] = seats[a]
    for seat in range(2 * slot_count):
        holder = sum(jnp.where(seats[a] == seat, a + 1, 0) for a in range(atoms))
        pairs[1, seat] = holder
    zero_row = jnp.zeros((1, funcs), f32)
    half = 16 if share % 16 == 0 else share

    def copies_from(source, g, s, piece):
        found = []
        for h in range(share // half) if piece is None else (piece,):
            rs = pl.ds(pl.multiple_of(g * share + h * half, 8), half)
            for side, start, target in ((0, planes - 2, right), (1, 0, left)):
                found.append(
                    pltpu.make_async_remote_copy(
                        src_ref=source.at[pl.ds(start, 2), rs],
                        dst_ref=halo.at[g, s, side, h],
                        send_sem=send_sem.at[g, side, h],
                        recv_sem=recv_sem.at[g, s, side, h],
                        device_id={"slab": target},
                        device_id_type=MESH,
                    )
                )
        return found

    pl.semaphore_wait(barrier, bands + 1)
    for g in range(groups):
        for copy in copies_from(even, g, 0, None):
            copy.start()

    quad = 4
    places = [plane_ref[a] - me * planes for a in range(atoms)]
    order = sorted(range(1, bands), key=lambda d: abs(d - bands / 2))
    unit = min(width, points)
    units = width // unit

    def outgoing(g, d, u):
        rs = pl.ds(pl.multiple_of(g * share, share), share)
        target = lax.rem(my_band + d, bands)
        if width >= points:
            src = even.at[target * units + u, rs]
        else:
            per = points // width
            src = even.at[target // per, rs, pl.ds(pl.multiple_of(lax.rem(target, per) * width, 128), width)]
        return pltpu.make_async_remote_copy(
            src_ref=src,
            dst_ref=out_ref.at[my_band, rs, u * unit : (u + 1) * unit],
            send_sem=out_sem.at[g, d - 1, u],
            recv_sem=in_sem.at[g, d - 1, u],
            device_id={"band": target},
            device_id_type=MESH,
        )

    def own(u):
        if width >= points:
            src = even.at[my_band * units + u]
        else:
            per = points // width
            src = even.at[my_band // per, :, pl.ds(pl.multiple_of(lax.rem(my_band, per) * width, 128), width)]
        return pltpu.make_async_copy(src, out_ref.at[my_band, :, u * unit : (u + 1) * unit], own_sem.at[u])

    def group_step(g, first):
        rs = pl.ds(first, share)

        def split_plane(x, c):
            high, low = halves(even[x, rs])
            split[x, :share] = high
            split[x, share:] = low
            return c

        lax.fori_loop(0, planes, split_plane, 0)

        def step(s, cur, nxt):
            scale = scal_ref[2 * s]
            pull = scal_ref[2 * s + 1]
            def pair(q, c):
                holders = [pairs[1, 2 * q + m] for m in range(2)]
                atom = [jnp.maximum(holder - 1, 0) for holder in holders]
                k = jnp.clip(kind_ref[atom[0]], 0, kinds - 1)
                places = [jnp.clip(plane_ref[atom[m]] - me * planes, 0, planes - depth) for m in range(2)]
                both = jnp.concatenate(
                    [jnp.concatenate([split[p + j] for j in range(depth)], axis=1) for p in places], axis=0
                )
                r = jnp.dot(both, table[k], preferred_element_type=f32)
                stack = []
                for m in range(2):
                    at = m * 2 * share
                    coupled = r[at : at + share, :funcs] + (
                        r[at : at + share, funcs:] + r[at + share : at + 2 * share, :funcs]
                    )
                    coef = jnp.where(holders[m] > 0, coef_ref[pl.ds(atom[m], 1)], zero_row)
                    for value in halves(coupled * coef):
                        stack.append(jnp.concatenate([value, value], axis=1))
                stack = jnp.concatenate(stack, axis=0)
                for j in range(depth):
                    r = jnp.dot(stack, back[k, :, j * points : (j + 1) * points], preferred_element_type=f32)
                    for m in range(2):
                        at = m * 2 * share
                        spread[2 * q + m, j + 1] = r[at : at + share] + r[at + share : at + 2 * share]
                return c

            lax.fori_loop(0, slot_count, pair, 0, unroll=True)

            seat_of = [pairs[0, a] for a in range(atoms)]
            slots = {x: [jnp.clip(x - places[a], -1, depth) + 1 for a in range(atoms)] for x in range(planes)}

            def quads(xs, take, first_row, count):
                both = jnp.concatenate(
                    [split[x, base + first_row : base + first_row + count] for x in xs for base in (0, share)], axis=0
                )
                r = jnp.dot(both, lap[...], preferred_element_type=f32)
                piece = min(16, share)
                span = min(256, points)
                for r0, l0 in [(r0, l0) for r0 in range(first_row, first_row + count, piece) for l0 in range(0, points, span)]:
                    ls = slice(l0, l0 + span)
                    fs = {}
                    for x in xs:
                        for d in (-2, -1, 0, 1, 2):
                            if x + d not in fs:
                                fs[x + d] = take(x + d, r0, piece, ls)
                    for i, x in enumerate(xs):
                        base = i * 2 * count + r0 - first_row
                        total = (r[base : base + piece, ls] + r[base + count : base + count + piece, ls]) * (-0.5 / 12.0)
                        total = total + (pot_ref[pl.ds(x, 1), ls] + (1.25 - centre)) * fs[x]
                        total = total + (fs[x - 1] + fs[x + 1]) * (-2.0 / 3.0) + (fs[x - 2] + fs[x + 2]) * (1.0 / 24.0)
                        for a in range(atoms):
                            total = total + spread[seat_of[a], slots[x][a], r0 : r0 + piece, ls]
                        at = (x, pl.ds(first + r0, piece), ls)
                        fresh = scale * total - pull * nxt[at]
                        nxt[at] = fresh
                        high, low = halves(fresh)
                        split[x, r0 : r0 + piece, ls] = high
                        split[x, share + r0 : share + r0 + piece, ls] = low

            def take(x, r0, piece, ls):
                if x < 0:
                    return halo[g, s, 0, r0 // half, x + 2, r0 % half : r0 % half + piece, ls]
                if x >= planes:
                    return halo[g, s, 1, r0 // half, x - planes, r0 % half : r0 % half + piece, ls]
                return cur[x, pl.ds(first + r0, piece), ls]

            def before(h):
                for copy in copies_from(cur, g, s, h):
                    copy.wait()

            def after(h):
                @pl.when(s + 1 < ORDER)
                def _():
                    for copy in copies_from(nxt, g, s + 1, h):
                        copy.start()

            for h in range(share // half):
                before(h)
                quads([0, 1, planes - 2, planes - 1], take, h * half, half)
                after(h)
                if h == 0:
                    for x0 in range(2, planes - 2, quad):
                        quads(list(range(x0, min(x0 + quad, planes - 2))), take, 0, share)

        def two(i, c):
            step(2 * i, even, odd)
            step(2 * i + 1, odd, even)
            return c

        lax.fori_loop(0, ORDER // 2, two, 0)

    def run_group(g, c):
        group_step(g, pl.multiple_of(g * share, share))
        for d in order:
            for u in range(units):
                outgoing(g, d, u).start()
        return c

    lax.fori_loop(0, groups, run_group, 0)
    for u in range(units):
        own(u).start()
    for g in range(groups):
        for d in order:
            for u in range(units):
                outgoing(g, d, u).wait()
    for u in range(units):
        own(u).wait()


def filter_call(plane, kind, cut, top, orb, pot, coef, proj, groups):
    rows, planes, points = orb.shape
    atoms = coef.shape[0]
    kinds, block, funcs = proj.shape
    depth = block // points
    bands = lax.axis_size("band")
    share = rows // groups
    width = planes * points // bands
    units = max(width // points, 1)
    half = 16 if share % 16 == 0 else share
    smem = pl.BlockSpec(memory_space=pltpu.SMEM)
    vmem = pl.BlockSpec(memory_space=pltpu.VMEM)
    hbm = pl.BlockSpec(memory_space=pl.ANY)
    dma = pltpu.SemaphoreType.DMA
    return pl.pallas_call(
        functools.partial(filter_kernel, groups),
        out_shape=jax.ShapeDtypeStruct((bands, rows, planes * points // bands), f32),
        in_specs=[smem] * 4 + [hbm, vmem, vmem, hbm],
        out_specs=vmem,
        scratch_shapes=[
            pltpu.VMEM((kinds, block, 2 * funcs), bf16),
            pltpu.VMEM((kinds, 2 * funcs, block), bf16),
            pltpu.VMEM((points, points), bf16),
            pltpu.VMEM((planes, rows, points), f32),
            pltpu.VMEM((planes, rows, points), f32),
            pltpu.VMEM((planes, 2 * share, points), bf16),
            pltpu.VMEM((2 * pair_slots(atoms, kinds), depth + 2, share, points), f32),
            pltpu.VMEM((groups, ORDER, 2, share // half, 2, half, points), f32),
            pltpu.VMEM((kinds, block, funcs), f32),
            pltpu.SMEM((2, max(atoms, 2 * pair_slots(atoms, kinds))), jnp.int32),
            pltpu.SMEM((2 * ORDER,), f32),
            dma((planes,)),
            dma((kinds,)),
            dma((units,)),
            dma((groups, 2, share // half)),
            dma((groups, ORDER, 2, share // half)),
            dma((groups, bands - 1, units)),
            dma((groups, bands - 1, units)),
        ],
        compiler_params=pltpu.CompilerParams(
            collective_id=0, has_side_effects=True, vmem_limit_bytes=60 * 1024 * 1024
        ),
        name="cheb_filter",
    )(plane, kind, cut, top, orb, pot, coef, proj)


def invert_block(t_ref, cols_ref, nb):
    lanes = lax.broadcasted_iota(jnp.int32, (micro, nb), 1)
    subs = lax.broadcasted_iota(jnp.int32, (micro, nb), 0)
    for k in range(0, nb, micro):
        inside = (lanes >= k) & (lanes < k + micro)
        head = t_ref[k : k + micro, :]
        for t in range(micro):
            cols_ref[t] = jnp.broadcast_to(head[:, k + t : k + t + 1], (micro, nb))
        rows = [
            jnp.where(inside, (lanes == k + t).astype(f32), jnp.broadcast_to(t_ref[k + t : k + t + 1, :], (micro, nb)))
            for t in range(micro)
        ]
        e = {
            (s, t): jnp.broadcast_to(cols_ref[t, s : s + 1, :], (micro, nb))
            for t in range(micro)
            for s in range(t, micro)
        }
        link, inv = {}, []
        for t in range(micro):
            inv.append(1.0 / e[t, t])
            for s in range(t + 1, micro):
                link[s, t] = e[s, t] * inv[t]
            for s in range(t + 1, micro):
                for u in range(t + 1, s + 1):
                    e[s, u] = e[s, u] - link[s, t] * e[u, t]
                rows[s] = rows[s] - link[s, t] * rows[t]
        solved = [rows[t] * inv[t] for t in range(micro)]
        for s in range(micro - 1, 0, -1):
            for t in range(s):
                solved[t] = solved[t] - link[s, t] * solved[s]
        for i in range(k + micro, nb, micro):
            tile = t_ref[i : i + micro, :]
            parts = [jnp.broadcast_to(tile[:, k + t : k + t + 1], (micro, nb)) * solved[t] for t in range(micro)]
            while len(parts) > 1:
                parts = [parts[j] + parts[j + 1] for j in range(0, len(parts), 2)]
            t_ref[i : i + micro, :] = jnp.where(inside, 0.0, tile) - parts[0]
        final = jnp.zeros((micro, nb), f32)
        for t in range(micro):
            final = jnp.where(subs == t, rows[t] * lax.rsqrt(e[t, t]), final)
        t_ref[k : k + micro, :] = jnp.where(lanes < k + micro, final, 0.0)


def factor_body(nb, a_ref, w_ref, t_ref, cols_ref, complete):
    n = w_ref.shape[0]
    nt = (((1,), (1,)), ((), ()))
    count = n // nb

    def one(b, c):
        at = pl.ds(pl.multiple_of(b * nb, nb), nb)
        t_ref[...] = a_ref[at, at]
        invert_block(t_ref, cols_ref, nb)
        pl.when(b == 0)(complete)
        for i in range(count):

            @pl.when(b == i)
            def _():
                lo, hi = i * nb, (i + 1) * nb
                inverse = t_ref[...]
                w_ref[lo:hi, lo:hi] = inverse
                if hi < n:
                    w_ref[lo:hi, hi:] = jnp.zeros((nb, n - hi), f32)
                    panel = lax.dot_general(a_ref[hi:, lo:hi], inverse, nt, precision=highest, preferred_element_type=f32)
                    a_ref[hi:, lo:hi] = panel
                    a_ref[hi:, hi:] = a_ref[hi:, hi:] - lax.dot_general(
                        panel, panel, nt, precision=highest, preferred_element_type=f32
                    )
                if lo > 0:
                    mixed = jnp.dot(a_ref[lo:hi, :lo], w_ref[:lo, :lo], precision=highest, preferred_element_type=f32)
                    w_ref[lo:hi, :lo] = -jnp.dot(inverse, mixed, precision=highest, preferred_element_type=f32)

        return c

    lax.fori_loop(0, count, one, 0)


def orthogonal_kernel(
    nb, point_total, f_ref, w_ref, stack, pack, first, part, second, full, a_ref, t_ref, cols_ref,
    pair_sems, sum_send, sum_recv, gather_send, gather_recv, relay_send, relay_recv,
):
    n = w_ref.shape[0]
    count = n // nb
    slabs, bands = lax.axis_size("slab"), lax.axis_size("band")
    my_slab, my_band = lax.axis_index("slab"), lax.axis_index("band")
    lines = slabs // 2
    chips = bands * lines
    core, chip = lax.rem(my_slab, 2), my_band * lines + my_slab // 2
    partner = my_slab + 1 - 2 * core
    sections = gram_sections(count, nb, chips)

    barrier = pltpu.get_barrier_semaphore()

    def place(d):
        other = lax.rem(chip + d, chips)
        return other, {"band": other // lines, "slab": lax.rem(other, lines) * 2 + core}

    def greet(d, c):
        pl.semaphore_signal(barrier, inc=1, device_id=place(d)[1], device_id_type=MESH)
        return c

    pl.semaphore_signal(barrier, inc=1, device_id={"slab": partner}, device_id_type=MESH)
    lax.fori_loop(1, chips, greet, 0)

    for i in range(count):
        rows = pl.ds(i * nb, nb)
        high, low = halves(f_ref[rows, :])
        stack[i, :nb] = high
        stack[i, nb:] = low
    for start, size, blocks in sections:
        at = start
        for i, j in blocks:
            r = lax.dot_general(stack[i], stack[j], (((1,), (1,)), ((), ())), preferred_element_type=f32)
            r = (r[:nb, :nb] + r[nb:, nb:]) + (r[:nb, nb:] + r[nb:, :nb])
            pack[at : at + nb] = r * (1.0 / point_total)
            at += nb
        if at < start + size:
            pack[at : start + size] = jnp.zeros((start + size - at, nb), f32)
    a_ref[...] = jnp.zeros((n, n), f32)

    pl.semaphore_wait(barrier, chips)

    def span(start, length):
        return pl.ds(pl.multiple_of(start, 8), length)

    def each(first_index, action):
        def body(d, c):
            action(d)
            return c

        lax.fori_loop(first_index, chips, body, 0)

    class Section:
        def __init__(self, index):
            self.index = index
            start, size, self.blocks = sections[index]
            self.start, self.deep = start, size // 2
            self.thin = self.deep // chips
            self.low = start // 2
            self.base = start + core * self.deep
            self.row = sum(sections[i][1] for i in range(index)) // 2 // chips

        def swap(self):
            return pltpu.make_async_remote_copy(
                src_ref=pack.at[span(self.start + (1 - core) * self.deep, self.deep)],
                dst_ref=first.at[pl.ds(self.low, self.deep)],
                send_sem=pair_sems.at[self.index, 0], recv_sem=pair_sems.at[self.index, 1],
                device_id={"slab": partner}, device_id_type=MESH,
            )

        def combine(self):
            own = pl.ds(self.low, self.deep)
            part[own] = pack[span(self.base, self.deep)] + first[own]

        def scatter(self, d):
            other, device = place(d)
            return pltpu.make_async_remote_copy(
                src_ref=part.at[span(self.low + other * self.thin, self.thin)],
                dst_ref=second.at[d - 1, self.row : self.row + self.thin],
                send_sem=sum_send.at[self.index, d - 1], recv_sem=sum_recv.at[self.index, d - 1],
                device_id=device, device_id_type=MESH,
            )

        def mine(self, c):
            return span(self.base + c * self.thin, self.thin)

        def total(self):
            def accumulate(d, value):
                return value + second[d - 1, self.row : self.row + self.thin]

            full[self.mine(chip)] = lax.fori_loop(
                1, chips, accumulate, part[span(self.low + chip * self.thin, self.thin)]
            )

        def gather(self, d):
            return pltpu.make_async_remote_copy(
                src_ref=full.at[self.mine(chip)], dst_ref=full.at[self.mine(chip)],
                send_sem=gather_send.at[self.index, d - 1], recv_sem=gather_recv.at[self.index, d - 1],
                device_id=place(d)[1], device_id_type=MESH,
            )

        def relay(self, d):
            rows = self.mine(lax.rem(chip + chips - d, chips))
            return pltpu.make_async_remote_copy(
                src_ref=full.at[rows], dst_ref=full.at[rows], send_sem=relay_send.at[self.index, d],
                recv_sem=relay_recv.at[self.index, d], device_id={"slab": partner}, device_id_type=MESH,
            )

        def publish(self):
            self.total()
            each(1, lambda d: self.gather(d).start())
            self.relay(0).start()

        def finish(self):
            def pass_on(d):
                self.gather(d).wait()
                self.relay(d).start()

            each(1, pass_on)
            each(0, lambda d: self.relay(d).wait())
            at = self.start
            for i, j in self.blocks:
                a_ref[i * nb : (i + 1) * nb, j * nb : (j + 1) * nb] = full[at : at + nb]
                at += nb

    parts = [Section(index) for index in range(len(sections))]
    for section in parts:
        section.swap().start()
    for section in parts:
        section.swap().wait()
        section.combine()
        each(1, lambda d: section.scatter(d).start())
    for section in parts:
        each(1, lambda d: section.scatter(d).wait())
        section.publish()
    parts[0].finish()

    def complete():
        for section in parts[1:]:
            section.finish()

    factor_body(nb, a_ref, w_ref, t_ref, cols_ref, complete)


def gram_sections(count, nb, chips):
    unit = 16 * chips
    found, start = [], 0
    for blocks in (
        [(i, 0) for i in range(count)],
        [(i, j) for j in range(1, count) for i in range(j, count)],
    ):
        size = (len(blocks) * nb + unit - 1) // unit * unit
        if blocks:
            found.append((start, size, blocks))
            start += size
    return found


def inverse_factor(grid_layout):
    n, width = grid_layout.shape
    nb = 128 if n % 128 == 0 else n
    slabs, bands = lax.axis_size("slab"), lax.axis_size("band")
    chips = bands * slabs // 2
    count = n // nb
    sections = gram_sections(count, nb, chips)
    total = sum(size for _, size, _ in sections)
    parts = len(sections)
    vmem = pl.BlockSpec(memory_space=pltpu.VMEM)
    dma = pltpu.SemaphoreType.DMA
    return pl.pallas_call(
        functools.partial(orthogonal_kernel, nb, width * slabs * bands),
        out_shape=jax.ShapeDtypeStruct((n, n), f32),
        in_specs=[vmem],
        out_specs=vmem,
        scratch_shapes=[
            pltpu.VMEM((count, 2 * nb, width), bf16),
            pltpu.VMEM((total, nb), f32),
            pltpu.VMEM((total // 2, nb), f32),
            pltpu.VMEM((total // 2, nb), f32),
            pltpu.VMEM((chips - 1, total // 2 // chips, nb), f32),
            pltpu.VMEM((total, nb), f32),
            pltpu.VMEM((n, n), f32),
            pltpu.VMEM((nb, nb), f32),
            pltpu.VMEM((micro, micro, nb), f32),
            dma((parts, 2)),
            dma((parts, chips - 1)),
            dma((parts, chips - 1)),
            dma((parts, chips - 1)),
            dma((parts, chips - 1)),
            dma((parts, chips)),
            dma((parts, chips)),
        ],
        compiler_params=pltpu.CompilerParams(
            collective_id=1, has_side_effects=True, vmem_limit_bytes=32 * 1024 * 1024
        ),
        name="gram_factor",
    )(grid_layout)


def local(
    orbitals, potential, projectors, atom_kind, atom_plane, atom_coef, filter_cut, filter_top
):
    rows = orbitals.shape[0]
    filtered = filter_call(
        atom_plane, atom_kind, filter_cut, filter_top, orbitals, potential, atom_coef, projectors, 2 if rows % 32 == 0 else 1
    )
    grid_layout = filtered.reshape(-1, filtered.shape[2])
    factor_inverse = inverse_factor(grid_layout)
    return jnp.dot(factor_inverse, grid_layout, precision=lax.Precision.HIGH)


def solution(mesh):
    in_specs = (
        P("band", "slab", None),
        P("slab", None),
        P(),
        P("slab"),
        P("slab"),
        P("slab", None),
        P(),
        P(),
    )
    out_specs = P(None, ("slab", "band"))
    return jax.shard_map(local, mesh=mesh, in_specs=in_specs, out_specs=out_specs, check_vma=False)
```
